512 devices in a mesh: tile: 32 (over x, y), depth: 16 (over z, core).
Axes of the slice: x: 4, y: 8, z: 8, core: 2. Of those that a mesh axis runs over, the one named last changes fastest.
Arguments:
- samples: bfloat16 [16, 16, 16384, 128], P('depth', None, 'tile'), may hold values from -6 to 6
- opacity: float32 [16, 16, 16384], P('depth', None, 'tile'), may hold values from 0.004 to 0.06
- counts: int32 [16, 16384], P('depth', 'tile'), may hold values from 0 to 16
- depth_order: int32 [32, 16], P('tile'), may hold values from 0 to 15, each once within a row
- target: float32 [16384, 128], P(('tile', 'depth')), may hold values from -6 to 6
- weight_in: bfloat16 [16, 128, 256], P('depth'), may hold values from -0.5 to 0.5
- weight_out: bfloat16 [16, 256, 128], P('depth'), may hold values from -1.5 to 1.5
Outputs:
- pixels: float32 [16384, 128], P(('tile', 'depth'))
- grad_in: float32 [16, 128, 256], P('depth', 'tile')
- grad_out: float32 [16, 256, 128], P('depth', 'tile')
The draws below stay inside these ranges and needn't reach their ends.
Inputs may be any that keep to these rules, and one draw needn't show every extreme that they name: `depth_order`: each row holds every brick rank 0 to 15 once.
All inputs are finite; a program needn't handle non-finite values.
Results may differ from the reference program's by a relative error of at most 0.0025.
Values sent between devices are 32-bit elements; how exact they have to be, the bound alone decides.
A program may use at most 64 MiB of HBM per device.

```python
import math
import jax
import jax.numpy as jnp
from jax import lax

ENC = 128
HID = 256
FEAT = 128
SAMPLES = 16
RAYS_TILE = 512
TILES = 32
BRICKS = 16
RAYS = 16384


def set_ends(result, own_key, low, top_value):
    longest = result.shape.index(max(result.shape))
    spots = []
    for shift in (0, 1):
        where = [jax.random.randint(jax.random.fold_in(own_key, axis), (), 0, length) for axis, length in enumerate(result.shape)]
        where[longest] = (where[longest] + shift) % result.shape[longest]
        spots.append(tuple(where))
    return result.at[spots[0]].set(low).at[spots[1]].set(top_value)


def shard_levels(own_key, dims, shards, low, largest):
    factor_of, own = 1.0, jax.random.fold_in(own_key, 6)
    for position, blocks in shards:
        steps = jnp.exp(jax.random.uniform(jax.random.fold_in(own, position), (blocks,), jnp.float32, low / len(shards), largest / len(shards)))
        factor_of = factor_of * jnp.repeat(steps, dims[position] // blocks).reshape([-1 if axis == position else 1 for axis in range(len(dims))])
    return factor_of


def scatter_about(key, dims, width, limit, shards=(), dtype=jnp.bfloat16):
    level = shard_levels(key, dims, shards, -0.22, 0.18) if shards else 1.0
    values = jax.random.normal(key, dims, jnp.float32) * width * level
    return jnp.minimum(jnp.maximum(values, -limit), limit).astype(dtype)


def setup_inputs(seed: int = 0) -> dict:
    keys = jax.random.split(jax.random.key(seed), 8)
    samples = scatter_about(keys[0], (BRICKS, SAMPLES, RAYS, ENC), 1.0, 6.0, ((0, 16), (2, 32)))
    opacity = jnp.clip(jnp.exp(math.log(0.06) - 2.70805 * jax.random.uniform(keys[1], (BRICKS, SAMPLES, RAYS), jnp.float32) ** shard_levels(keys[1], (BRICKS, SAMPLES, RAYS), ((0, 16), (2, 32)), -0.2, 0.2)), 0.004, 0.06)
    counts = set_ends(jax.random.randint(keys[2], (BRICKS, RAYS), 0, 17), jax.random.fold_in(keys[2], 1), 0, 16).astype(jnp.int32)
    depth_order = jax.vmap(lambda own: jax.random.permutation(own, BRICKS))(jax.random.split(keys[3], TILES)).reshape((TILES, BRICKS)).astype(jnp.int32)
    target = scatter_about(keys[4], (RAYS, FEAT), 1.0, 6.0, ((0, 512),), jnp.float32)
    weight_in = scatter_about(keys[5], (BRICKS, ENC, HID), ENC ** -0.5, 0.5, ((0, 16),))
    weight_out = scatter_about(keys[6], (BRICKS, HID, FEAT), (HID // 16) ** -0.5, 1.5, ((0, 16),))
    return dict(samples=samples, opacity=opacity, counts=counts, depth_order=depth_order, target=target, weight_in=weight_in, weight_out=weight_out)


def reference(samples, opacity, counts, depth_order, target, weight_in, weight_out):
    slot_index = lax.broadcasted_iota(jnp.int32, opacity.shape, 1)
    living = (slot_index < counts[:, None, :]).astype(jnp.float32)
    kept = 1.0 - opacity * living
    ones_row = jnp.ones((opacity.shape[0], 1, opacity.shape[2]), jnp.float32)
    through = jnp.cumprod(jnp.concatenate([ones_row, kept[:, :-1, :]], axis=1), axis=1)
    contrib = living * opacity * through
    passing = jnp.prod(kept, axis=1)
    tile_of = (jnp.arange(RAYS) // RAYS_TILE).astype(jnp.int32)
    brick_rank = depth_order[tile_of, :].T
    in_front = brick_rank[None, :, :] < brick_rank[:, None, :]
    veiling = jnp.prod(jnp.where(in_front, passing[None, :, :], 1.0), axis=1)

    def forward(packed):
        inputs, share, first, second = packed
        flat = inputs.reshape(SAMPLES * RAYS, ENC)
        before_act = jnp.dot(flat, first, preferred_element_type=jnp.float32)
        hidden = jnp.maximum(before_act, 0.0).astype(jnp.bfloat16)
        radiance = jnp.dot(hidden, second, preferred_element_type=jnp.float32).reshape(SAMPLES, RAYS, FEAT)
        return jnp.sum(share[:, :, None] * radiance, axis=0)

    factor = contrib * veiling[:, None, :]
    terms = lax.map(forward, (samples, factor, weight_in, weight_out))
    pixels = jnp.sum(terms, axis=0)
    pixel_grad = pixels - target

    def backward(packed):
        inputs, share, first, second = packed
        flat = inputs.reshape(SAMPLES * RAYS, ENC)
        before_act = jnp.dot(flat, first, preferred_element_type=jnp.float32)
        hidden = jnp.maximum(before_act, 0.0).astype(jnp.bfloat16)
        feat_grad = (share[:, :, None] * pixel_grad[None, :, :]).astype(jnp.bfloat16).reshape(SAMPLES * RAYS, FEAT)
        out_grad = jnp.dot(hidden.T, feat_grad, preferred_element_type=jnp.float32)
        hidden_grad = jnp.dot(feat_grad, second.T, preferred_element_type=jnp.float32)
        hidden_grad = jnp.where(before_act > 0.0, hidden_grad, 0.0).astype(jnp.bfloat16)
        in_grad = jnp.dot(flat.T, hidden_grad, preferred_element_type=jnp.float32)
        return in_grad, out_grad

    grad_in, grad_out = lax.map(backward, (samples, factor, weight_in, weight_out))
    return pixels, grad_in, grad_out
```

```python
import jax
import jax.numpy as jnp
from jax import lax
from jax.experimental import pallas as pl
from jax.experimental.pallas import tpu as pltpu
from jax.sharding import PartitionSpec as P

ENC, HID, FEAT, SLOTS, RAYS = 128, 256, 128, 16, 512
BRICKS, OWN = 16, 32
ZS, XS, YS = 8, 4, 8
PAIR = 2 * OWN
ROWS = SLOTS * PAIR
MESH = pl.DeviceIdType.MESH
F32, BF16 = jnp.float32, jnp.bfloat16


def dot(a, b):
    return jnp.dot(a, b, preferred_element_type=F32)


def dot_t(a, b):
    return lax.dot_general(a, b, (((1,), (1,)), ((), ())), preferred_element_type=F32)


def split(a):
    high = a.astype(BF16)
    return high, (a - high.astype(F32)).astype(BF16)


def far_first(k):
    return lax.rem(4 + (1 - 2 * lax.rem(k, 2)) * lax.div(k + 1, 2) + 8, 8)


def kernel(
    samples_h, opacity_h, counts_h, order_h, target_h, first_h, second_h,
    pixels_o, grad_in_o, grad_out_o,
    xs, op, cnt, order, tgt, w1, w2,
    passed, ct, vt, hid, total, wsend, wrecv, pgs, fst, gin, gout,
    xin, xout, ysin, ysout, yin, yout,
    load_sem, p_send, p_recv, w_send, w_recv, g_send, g_recv, f_send, f_recv,
    x_send, x_recv, y_send, y_recv,
):
    tile = lax.axis_index("tile")
    own = lax.axis_index("depth")
    zi, core = lax.div(own, 2), lax.rem(own, 2)
    xi, yi = lax.div(tile, YS), lax.rem(tile, YS)
    partner = 2 * zi + 1 - core

    barrier = pltpu.get_barrier_semaphore()

    def greet(t, d):
        pl.semaphore_signal(
            barrier, inc=1, device_id={"tile": t, "depth": d}, device_id_type=MESH
        )

    @pl.loop(1, BRICKS)
    def _(j):
        greet(tile, lax.rem(own + j, BRICKS))

    @pl.loop(1, XS)
    def _(j):
        greet(lax.rem(xi + j, XS) * YS + yi, own)

    @pl.loop(1, YS)
    def _(j):
        greet(xi * YS + lax.rem(yi + j, YS), own)

    loads = [
        pltpu.make_async_copy(a, b, load_sem.at[i])
        for i, (a, b) in enumerate(
            [
                (opacity_h.at[0], op), (counts_h, cnt), (first_h.at[0], w1),
                (samples_h.at[0], xs), (second_h.at[0], w2), (order_h, order),
                (target_h, tgt),
            ]
        )
    ]
    for load in loads:
        load.start()

    def remote(src, dst, send, recv, t, d):
        return pltpu.make_async_remote_copy(
            src_ref=src, dst_ref=dst, send_sem=send, recv_sem=recv,
            device_id={"tile": t, "depth": d}, device_id_type=MESH,
        )

    loads[0].wait()
    loads[1].wait()
    slot = lax.broadcasted_iota(jnp.int32, (SLOTS, RAYS), 0)
    living = jnp.where(slot < cnt[...], 1.0, 0.0).astype(F32)
    alpha = op[...] * living
    kept = 1.0 - alpha
    through = jnp.ones((1, RAYS), F32)
    rows = []
    for s in range(SLOTS):
        rows.append(alpha[s : s + 1] * through)
        through = through * kept[s : s + 1]
    contrib = jnp.concatenate(rows + [jnp.zeros((128 - SLOTS, RAYS), F32)], axis=0)
    passed[own] = through
    ct[...] = contrib.T

    pl.semaphore_wait(barrier, BRICKS - 1 + XS - 1 + YS - 1)

    def p_copy(d):
        return remote(passed.at[own], passed.at[own], p_send.at[d], p_recv.at[own], tile, d)

    @pl.loop(0, BRICKS - 1)
    def _(j):
        p_copy(lax.rem(own + 8 + lax.div(j + 1, 2) * (1 - 2 * lax.rem(j, 2)) + BRICKS, BRICKS)).start()

    loads[2].wait()
    loads[3].wait()
    loads[4].wait()

    def w_copy(d):
        return remote(wsend.at[d], wrecv.at[own], w_send.at[d], w_recv.at[own], tile, d)

    def forward(zt):
        first_ray = pl.multiple_of(zt * PAIR, PAIR)
        rays = pl.ds(first_ray, PAIR)
        flat = xs[:, rays, :].reshape(ROWS, ENC)
        act = jnp.maximum(dot(flat, w1[...]), 0.0)
        hid[zt] = act.astype(BF16)
        cols = ct[rays, :]
        acc = jnp.zeros((PAIR, HID), F32)
        for s in range(SLOTS):
            acc = acc + act[s * PAIR : (s + 1) * PAIR] * cols[:, s : s + 1]
        total[rays, :] = acc
        high, low = split(acc)
        term = dot(high, w2[...]) + dot(low, w2[...])
        wsend[pl.ds(2 * zt, 2)] = term.reshape(2, OWN, FEAT)

    @pl.loop(0, ZS - 1)
    def _(k):
        zt = lax.rem(zi + far_first(k), ZS)
        forward(zt)
        w_copy(2 * zt).start()
        w_copy(2 * zt + 1).start()

    forward(zi)
    w_copy(partner).start()
    wrecv[own] = wsend[own]

    @pl.loop(0, ZS)
    def _(zt):
        rays = pl.ds(pl.multiple_of(zt * PAIR, PAIR), PAIR)
        cols = ct[rays, :]
        parts = []
        for s in range(SLOTS):
            parts.append((xs[s, rays, :].astype(F32) * cols[:, s : s + 1]).astype(BF16))
        fst[zt] = jnp.concatenate(parts, axis=0).T

    loads[5].wait()
    loads[6].wait()

    @pl.loop(1, BRICKS)
    def _(j):
        d = lax.rem(own + j, BRICKS)
        remote(passed.at[d], passed.at[d], p_send.at[d], p_recv.at[d], tile, d).wait_recv()

    every = jnp.concatenate([passed[b] for b in range(BRICKS)], axis=0)
    rank = order[...].astype(F32)
    grid = (BRICKS, BRICKS)
    ranks = jnp.broadcast_to(rank, grid)
    eye = lax.broadcasted_iota(jnp.int32, grid, 0) == lax.broadcasted_iota(jnp.int32, grid, 1)
    rank_col = jnp.sum(jnp.where(eye, ranks, 0.0), axis=1, keepdims=True)
    veils = []
    for b in range(BRICKS):
        chosen = jnp.where(rank_col < rank[:, b : b + 1], every, 1.0)
        chosen = chosen[:8] * chosen[8:]
        chosen = chosen[:4] * chosen[4:]
        chosen = chosen[:2] * chosen[2:]
        veils.append(chosen[:1] * chosen[1:])
    veil = jnp.concatenate(veils, axis=0)
    brick = lax.broadcasted_iota(jnp.int32, (BRICKS, RAYS), 0)
    veil_own = jnp.sum(jnp.where(brick == own, veil, 0.0), axis=0, keepdims=True)
    vt[...] = jnp.concatenate([veil, veil_own, jnp.zeros((127 - BRICKS, RAYS), F32)], axis=0).T

    @pl.loop(1, BRICKS)
    def _(j):
        d = lax.rem(own + j, BRICKS)
        remote(wsend.at[d], wrecv.at[d], w_send.at[d], w_recv.at[d], tile, d).wait_recv()

    mine = vt[pl.ds(pl.multiple_of(own * OWN, OWN), OWN), :]
    pixels = jnp.zeros((OWN, FEAT), F32)
    for b in range(BRICKS):
        pixels = pixels + wrecv[b] * mine[:, b : b + 1]
    pixels_o[...] = pixels
    pgs[own] = pixels - tgt[...]

    def g_copy(d):
        return remote(pgs.at[own], pgs.at[own], g_send.at[d], g_recv.at[own], tile, d)

    def f_copy(b):
        return remote(pgs.at[b], pgs.at[b], f_send.at[b], f_recv.at[b], tile, partner)

    @pl.loop(0, ZS - 1)
    def _(k):
        g_copy(2 * lax.rem(zi + far_first(k), ZS) + core).start()

    g_copy(partner).start()

    gin[...] = jnp.zeros((ENC, HID), F32)
    gout[...] = jnp.zeros((HID, FEAT), F32)

    def backward(zt):
        rays = pl.ds(pl.multiple_of(zt * PAIR, PAIR), PAIR)
        grad = pgs[pl.ds(2 * zt, 2)].reshape(PAIR, FEAT)
        veil_col = vt[rays, BRICKS : BRICKS + 1]
        high, low = split(grad * veil_col)
        spread = (dot_t(high, w2[...]) + dot_t(low, w2[...])).astype(BF16)
        summed = total[rays, :].astype(BF16)
        gout[...] += dot(summed.T, high)
        parts = []
        for s in range(SLOTS):
            live = hid[zt, s * PAIR : (s + 1) * PAIR, :] > 0
            parts.append(jnp.where(live, spread, jnp.zeros_like(spread)))
        gin[...] += dot(fst[zt], jnp.concatenate(parts, axis=0))

    def wait_g(b):
        remote(pgs.at[b], pgs.at[b], g_send.at[b], g_recv.at[b], tile, b).wait_recv()

    wait_g(partner)
    backward(zi)

    def near_first(k):
        return lax.rem(zi + far_first(6 - k), ZS)

    @pl.loop(0, ZS - 1)
    def _(k):
        zt = near_first(k)
        wait_g(2 * zt + core)
        f_copy(2 * zt + core).start()

    @pl.loop(0, ZS - 1)
    def _(k):
        zt = near_first(k)
        f_copy(2 * zt + 1 - core).wait_recv()
        backward(zt)

    def x_copies(xt):
        t = xt * YS + yi
        rin, rout = pl.ds(pl.multiple_of(32 * xt, 32), 32), pl.ds(pl.multiple_of(64 * xt, 64), 64)
        return (
            remote(gout.at[rout], xout.at[xi], x_send.at[xt, 0], x_recv.at[xi, 0], t, own),
            remote(gin.at[rin], xin.at[xi], x_send.at[xt, 1], x_recv.at[xi, 1], t, own),
        )

    def x_arrivals(xt):
        t = xt * YS + yi
        rin, rout = pl.ds(pl.multiple_of(32 * xt, 32), 32), pl.ds(pl.multiple_of(64 * xt, 64), 64)
        return (
            remote(gout.at[rout], xout.at[xt], x_send.at[xt, 0], x_recv.at[xt, 0], t, own),
            remote(gin.at[rin], xin.at[xt], x_send.at[xt, 1], x_recv.at[xt, 1], t, own),
        )

    for j in (2, 1, 3):
        for copy in x_copies(lax.rem(xi + j, XS)):
            copy.start()
    xout[xi] = gout[pl.ds(pl.multiple_of(64 * xi, 64), 64), :]
    xin[xi] = gin[pl.ds(pl.multiple_of(32 * xi, 32), 32), :]
    for j in (1, 3, 2):
        for copy in x_arrivals(lax.rem(xi + j, XS)):
            copy.wait_recv()
    sum_out = xout[0] + xout[1] + xout[2] + xout[3]
    sum_in = xin[0] + xin[1] + xin[2] + xin[3]
    ysout[...] = sum_out.reshape(YS, 8, FEAT)
    for j in range(YS):
        ysin[j] = sum_in[4 * j : 4 * j + 4]

    def y_copies(yt):
        t = xi * YS + yt
        return (
            remote(ysout.at[yt], yout.at[yi], y_send.at[yt, 0], y_recv.at[yi, 0], t, own),
            remote(ysin.at[yt], yin.at[yi], y_send.at[yt, 1], y_recv.at[yi, 1], t, own),
        )

    def y_arrivals(yt):
        t = xi * YS + yt
        return (
            remote(ysout.at[yt], yout.at[yt], y_send.at[yt, 0], y_recv.at[yt, 0], t, own),
            remote(ysin.at[yt], yin.at[yt], y_send.at[yt, 1], y_recv.at[yt, 1], t, own),
        )

    @pl.loop(0, YS - 1)
    def _(k):
        for copy in y_copies(lax.rem(yi + far_first(k), YS)):
            copy.start()

    yout[yi] = ysout[yi]
    yin[yi] = ysin[yi]

    @pl.loop(1, YS)
    def _(j):
        for copy in y_arrivals(lax.rem(yi + j, YS)):
            copy.wait_recv()

    acc_out, acc_in = yout[0], yin[0]
    for j in range(1, YS):
        acc_out = acc_out + yout[j]
        acc_in = acc_in + yin[j]
    grad_out_o[0] = acc_out
    grad_in_o[0] = acc_in

    @pl.loop(1, BRICKS)
    def _(j):
        d = lax.rem(own + j, BRICKS)
        p_copy(d).wait_send()
        w_copy(d).wait_send()

    g_copy(partner).wait_send()

    @pl.loop(1, ZS)
    def _(j):
        d = 2 * lax.rem(zi + j, ZS) + core
        g_copy(d).wait_send()
        f_copy(d).wait_send()

    @pl.loop(1, XS)
    def _(j):
        for copy in x_copies(lax.rem(xi + j, XS)):
            copy.wait_send()

    @pl.loop(1, YS)
    def _(j):
        for copy in y_copies(lax.rem(yi + j, YS)):
            copy.wait_send()


def per_device(samples, opacity, counts, depth_order, target, weight_in, weight_out):
    any_space = pl.BlockSpec(memory_space=pl.ANY)
    vmem = pl.BlockSpec(memory_space=pltpu.VMEM)
    dma = pltpu.SemaphoreType.DMA
    return pl.pallas_call(
        kernel,
        out_shape=(
            jax.ShapeDtypeStruct((OWN, FEAT), F32),
            jax.ShapeDtypeStruct((1, 4, HID), F32),
            jax.ShapeDtypeStruct((1, 8, FEAT), F32),
        ),
        in_specs=[any_space] * 7,
        out_specs=(vmem, vmem, vmem),
        scratch_shapes=[
            pltpu.VMEM((SLOTS, RAYS, ENC), BF16),
            pltpu.VMEM((SLOTS, RAYS), F32),
            pltpu.VMEM((1, RAYS), jnp.int32),
            pltpu.VMEM((1, BRICKS), jnp.int32),
            pltpu.VMEM((OWN, FEAT), F32),
            pltpu.VMEM((ENC, HID), BF16),
            pltpu.VMEM((HID, FEAT), BF16),
            pltpu.VMEM((BRICKS, 1, RAYS), F32),
            pltpu.VMEM((RAYS, 128), F32),
            pltpu.VMEM((RAYS, 128), F32),
            pltpu.VMEM((ZS, ROWS, HID), BF16),
            pltpu.VMEM((RAYS, HID), F32),
            pltpu.VMEM((BRICKS, OWN, FEAT), F32),
            pltpu.VMEM((BRICKS, OWN, FEAT), F32),
            pltpu.VMEM((BRICKS, OWN, FEAT), F32),
            pltpu.VMEM((ZS, ENC, ROWS), BF16),
            pltpu.VMEM((ENC, HID), F32),
            pltpu.VMEM((HID, FEAT), F32),
            pltpu.VMEM((XS, 32, HID), F32),
            pltpu.VMEM((XS, 64, FEAT), F32),
            pltpu.VMEM((YS, 4, HID), F32),
            pltpu.VMEM((YS, 8, FEAT), F32),
            pltpu.VMEM((YS, 4, HID), F32),
            pltpu.VMEM((YS, 8, FEAT), F32),
            dma((7,)),
            dma((BRICKS,)), dma((BRICKS,)),
            dma((BRICKS,)), dma((BRICKS,)),
            dma((BRICKS,)), dma((BRICKS,)),
            dma((BRICKS,)), dma((BRICKS,)),
            dma((XS, 2)), dma((XS, 2)),
            dma((YS, 2)), dma((YS, 2)),
        ],
        compiler_params=pltpu.CompilerParams(collective_id=0, has_side_effects=True),
        name="field_step",
    )(samples, opacity, counts, depth_order, target, weight_in, weight_out)


def solution(mesh):
    placed = (
        P("depth", None, "tile", None),
        P("depth", None, "tile"),
        P("depth", "tile"),
        P("tile", None),
        P(("tile", "depth"), None),
        P("depth", None, None),
        P("depth", None, None),
    )
    return jax.shard_map(
        per_device,
        mesh=mesh,
        in_specs=placed,
        out_specs=(P(("tile", "depth"), None), P("depth", "tile", None), P("depth", "tile", None)),
        check_vma=False,
    )
```

```python
import jax
import jax.numpy as jnp
from jax import lax
from jax.experimental import pallas as pl
from jax.experimental.pallas import tpu as pltpu
from jax.sharding import PartitionSpec as P

ENC, HID, FEAT, SLOTS, RAYS = 128, 256, 128, 16, 512
BRICKS, OWN = 16, 32
EARLY = 4
ZS, XS, YS = 8, 4, 8
PAIR = 2 * OWN
ROWS = SLOTS * PAIR
MESH = pl.DeviceIdType.MESH
F32, BF16 = jnp.float32, jnp.bfloat16


def dot(a, b):
    return jnp.dot(a, b, preferred_element_type=F32)


def dot_t(a, b):
    return lax.dot_general(a, b, (((1,), (1,)), ((), ())), preferred_element_type=F32)


def split(a):
    high = a.astype(BF16)
    return high, (a - high.astype(F32)).astype(BF16)


def far_first(k):
    return lax.rem(4 + (1 - 2 * lax.rem(k, 2)) * lax.div(k + 1, 2) + 8, 8)


def kernel(
    samples_h, opacity_h, counts_h, order_h, target_h, first_h, second_h,
    pixels_o, grad_in_o, grad_out_o,
    xs, op, cnt, order, tgt, w1, w2,
    passed, ct, vt, hid, total, wsend, wrecv, pgs, fst, gin, gout,
    xin, xout, ysin, ysout, yin, yout,
    load_sem, chunk_sem, p_send, p_recv, w_send, w_recv, g_send, g_recv, f_send, f_recv,
    x_send, x_recv, y_send, y_recv,
):
    tile = lax.axis_index("tile")
    own = lax.axis_index("depth")
    zi, core = lax.div(own, 2), lax.rem(own, 2)
    xi, yi = lax.div(tile, YS), lax.rem(tile, YS)
    partner = 2 * zi + 1 - core

    loads = [
        pltpu.make_async_copy(a, b, load_sem.at[i])
        for i, (a, b) in enumerate(
            [
                (opacity_h.at[0], op), (counts_h, cnt), (first_h.at[0], w1),
                (second_h.at[0], w2), (order_h, order), (target_h, tgt),
            ]
        )
    ]
    for load in loads[:3]:
        load.start()

    def rays_of(zt):
        return pl.ds(pl.multiple_of(zt * PAIR, PAIR), PAIR)

    def fetch(k):
        rays = rays_of(lax.rem(zi + far_first(k), ZS))
        return pltpu.make_async_copy(samples_h.at[0, :, rays, :], xs.at[:, rays, :], chunk_sem.at[k])

    for k in range(ZS):
        fetch(k).start()
    for load in loads[3:]:
        load.start()

    barrier = pltpu.get_barrier_semaphore()

    def greet(t, d):
        pl.semaphore_signal(
            barrier, inc=1, device_id={"tile": t, "depth": d}, device_id_type=MESH
        )

    for j in range(1, BRICKS):
        greet(tile, lax.rem(own + j, BRICKS))
    for j in range(1, XS):
        greet(lax.rem(xi + j, XS) * YS + yi, own)
    for j in range(1, YS):
        greet(xi * YS + lax.rem(yi + j, YS), own)

    def remote(src, dst, send, recv, t, d):
        return pltpu.make_async_remote_copy(
            src_ref=src, dst_ref=dst, send_sem=send, recv_sem=recv,
            device_id={"tile": t, "depth": d}, device_id_type=MESH,
        )

    loads[0].wait()
    loads[1].wait()
    slot = lax.broadcasted_iota(jnp.int32, (SLOTS, RAYS), 0)
    living = jnp.where(slot < cnt[...], 1.0, 0.0).astype(F32)
    alpha = op[...] * living
    kept = 1.0 - alpha
    through = jnp.ones((1, RAYS), F32)
    rows = []
    for s in range(SLOTS):
        rows.append(alpha[s : s + 1] * through)
        through = through * kept[s : s + 1]
    contrib = jnp.concatenate(rows + [jnp.zeros((128 - SLOTS, RAYS), F32)], axis=0)
    passed[own] = through
    ct[...] = contrib.T

    def p_copy(d):
        return remote(passed.at[own], passed.at[own], p_send.at[d], p_recv.at[own], tile, d)

    loads[2].wait()
    loads[3].wait()

    def w_copy(d):
        return remote(wsend.at[d], wrecv.at[own], w_send.at[d], w_recv.at[own], tile, d)

    def forward(zt):
        rays = rays_of(zt)
        flat = xs[:, rays, :].reshape(ROWS, ENC)
        act = jnp.maximum(dot(flat, w1[...]), 0.0)
        hid[zt] = act.astype(BF16)
        cols = ct[rays, :]
        acc = jnp.zeros((PAIR, HID), F32)
        for s in range(SLOTS):
            acc = acc + act[s * PAIR : (s + 1) * PAIR] * cols[:, s : s + 1]
        total[rays, :] = acc
        high, low = split(acc)
        term = dot(high, w2[...]) + dot(low, w2[...])
        wsend[pl.ds(2 * zt, 2)] = term.reshape(2, OWN, FEAT)

    def send_pair(zt):
        w_copy(2 * zt).start()
        w_copy(2 * zt + 1).start()

    @pl.loop(0, EARLY)
    def _(k):
        fetch(k).wait()
        forward(lax.rem(zi + far_first(k), ZS))

    pl.semaphore_wait(barrier, BRICKS - 1 + XS - 1 + YS - 1)

    @pl.loop(0, BRICKS - 1)
    def _(j):
        p_copy(lax.rem(own + 8 + lax.div(j + 1, 2) * (1 - 2 * lax.rem(j, 2)) + BRICKS, BRICKS)).start()

    @pl.loop(0, EARLY)
    def _(k):
        send_pair(lax.rem(zi + far_first(k), ZS))

    @pl.loop(EARLY, ZS - 1)
    def _(k):
        zt = lax.rem(zi + far_first(k), ZS)
        fetch(k).wait()
        forward(zt)
        send_pair(zt)

    fetch(ZS - 1).wait()
    forward(zi)
    w_copy(partner).start()
    wrecv[own] = wsend[own]

    @pl.loop(0, ZS)
    def _(zt):
        rays = rays_of(zt)
        cols = ct[rays, :]
        parts = []
        for s in range(SLOTS):
            parts.append((xs[s, rays, :].astype(F32) * cols[:, s : s + 1]).astype(BF16))
        fst[zt] = jnp.concatenate(parts, axis=0).T

    loads[4].wait()
    loads[5].wait()

    @pl.loop(1, BRICKS)
    def _(j):
        d = lax.rem(own + j, BRICKS)
        remote(passed.at[d], passed.at[d], p_send.at[d], p_recv.at[d], tile, d).wait_recv()

    every = jnp.concatenate([passed[b] for b in range(BRICKS)], axis=0)
    rank = order[...].astype(F32)
    grid = (BRICKS, BRICKS)
    ranks = jnp.broadcast_to(rank, grid)
    eye = lax.broadcasted_iota(jnp.int32, grid, 0) == lax.broadcasted_iota(jnp.int32, grid, 1)
    rank_col = jnp.sum(jnp.where(eye, ranks, 0.0), axis=1, keepdims=True)
    veils = []
    for b in range(BRICKS):
        chosen = jnp.where(rank_col < rank[:, b : b + 1], every, 1.0)
        chosen = chosen[:8] * chosen[8:]
        chosen = chosen[:4] * chosen[4:]
        chosen = chosen[:2] * chosen[2:]
        veils.append(chosen[:1] * chosen[1:])
    veil = jnp.concatenate(veils, axis=0)
    brick = lax.broadcasted_iota(jnp.int32, (BRICKS, RAYS), 0)
    veil_own = jnp.sum(jnp.where(brick == own, veil, 0.0), axis=0, keepdims=True)
    vt[...] = jnp.concatenate([veil, veil_own, jnp.zeros((127 - BRICKS, RAYS), F32)], axis=0).T

    @pl.loop(1, BRICKS)
    def _(j):
        d = lax.rem(own + j, BRICKS)
        remote(wsend.at[d], wrecv.at[d], w_send.at[d], w_recv.at[d], tile, d).wait_recv()

    mine = vt[pl.ds(pl.multiple_of(own * OWN, OWN), OWN), :]
    pixels = jnp.zeros((OWN, FEAT), F32)
    for b in range(BRICKS):
        pixels = pixels + wrecv[b] * mine[:, b : b + 1]
    pixels_o[...] = pixels
    pgs[own] = pixels - tgt[...]

    def g_copy(d):
        return remote(pgs.at[own], pgs.at[own], g_send.at[d], g_recv.at[own], tile, d)

    def f_copy(b):
        return remote(pgs.at[b], pgs.at[b], f_send.at[b], f_recv.at[b], tile, partner)

    @pl.loop(0, ZS - 1)
    def _(k):
        g_copy(2 * lax.rem(zi + far_first(k), ZS) + core).start()

    g_copy(partner).start()

    gin[...] = jnp.zeros((ENC, HID), F32)
    gout[...] = jnp.zeros((HID, FEAT), F32)

    def backward(zt):
        rays = rays_of(zt)
        grad = pgs[pl.ds(2 * zt, 2)].reshape(PAIR, FEAT)
        veil_col = vt[rays, BRICKS : BRICKS + 1]
        high, low = split(grad * veil_col)
        spread = (dot_t(high, w2[...]) + dot_t(low, w2[...])).astype(BF16)
        summed = total[rays, :].astype(BF16)
        gout[...] += dot(summed.T, high)
        parts = []
        for s in range(SLOTS):
            live = hid[zt, s * PAIR : (s + 1) * PAIR, :] > 0
            parts.append(jnp.where(live, spread, jnp.zeros_like(spread)))
        gin[...] += dot(fst[zt], jnp.concatenate(parts, axis=0))

    def wait_g(b):
        remote(pgs.at[b], pgs.at[b], g_send.at[b], g_recv.at[b], tile, b).wait_recv()

    def near_first(k):
        return lax.rem(zi + far_first(6 - k), ZS)

    def relay(k):
        b = 2 * near_first(k) + core
        wait_g(b)
        f_copy(b).start()

    def settle(k):
        zt = near_first(k)
        f_copy(2 * zt + 1 - core).wait_recv()
        backward(zt)

    wait_g(partner)
    backward(zi)
    relay(0)

    @pl.loop(1, ZS - 1)
    def _(k):
        relay(k)
        settle(k - 1)

    settle(ZS - 2)

    def x_copies(xt):
        t = xt * YS + yi
        rin, rout = pl.ds(pl.multiple_of(32 * xt, 32), 32), pl.ds(pl.multiple_of(64 * xt, 64), 64)
        return (
            remote(gout.at[rout], xout.at[xi], x_send.at[xt, 0], x_recv.at[xi, 0], t, own),
            remote(gin.at[rin], xin.at[xi], x_send.at[xt, 1], x_recv.at[xi, 1], t, own),
        )

    def x_arrivals(xt):
        t = xt * YS + yi
        rin, rout = pl.ds(pl.multiple_of(32 * xt, 32), 32), pl.ds(pl.multiple_of(64 * xt, 64), 64)
        return (
            remote(gout.at[rout], xout.at[xt], x_send.at[xt, 0], x_recv.at[xt, 0], t, own),
            remote(gin.at[rin], xin.at[xt], x_send.at[xt, 1], x_recv.at[xt, 1], t, own),
        )

    for j in (2, 1, 3):
        for copy in x_copies(lax.rem(xi + j, XS)):
            copy.start()
    xout[xi] = gout[pl.ds(pl.multiple_of(64 * xi, 64), 64), :]
    xin[xi] = gin[pl.ds(pl.multiple_of(32 * xi, 32), 32), :]
    for j in (1, 3, 2):
        for copy in x_arrivals(lax.rem(xi + j, XS)):
            copy.wait_recv()
    sum_out = xout[0] + xout[1] + xout[2] + xout[3]
    sum_in = xin[0] + xin[1] + xin[2] + xin[3]
    ysout[...] = sum_out.reshape(YS, 8, FEAT)
    for j in range(YS):
        ysin[j] = sum_in[4 * j : 4 * j + 4]

    def y_copies(yt):
        t = xi * YS + yt
        return (
            remote(ysout.at[yt], yout.at[yi], y_send.at[yt, 0], y_recv.at[yi, 0], t, own),
            remote(ysin.at[yt], yin.at[yi], y_send.at[yt, 1], y_recv.at[yi, 1], t, own),
        )

    def y_arrivals(yt):
        t = xi * YS + yt
        return (
            remote(ysout.at[yt], yout.at[yt], y_send.at[yt, 0], y_recv.at[yt, 0], t, own),
            remote(ysin.at[yt], yin.at[yt], y_send.at[yt, 1], y_recv.at[yt, 1], t, own),
        )

    @pl.loop(0, YS - 1)
    def _(k):
        for copy in y_copies(lax.rem(yi + far_first(k), YS)):
            copy.start()

    yout[yi] = ysout[yi]
    yin[yi] = ysin[yi]

    @pl.loop(1, YS)
    def _(j):
        for copy in y_arrivals(lax.rem(yi + j, YS)):
            copy.wait_recv()

    acc_out, acc_in = yout[0], yin[0]
    for j in range(1, YS):
        acc_out = acc_out + yout[j]
        acc_in = acc_in + yin[j]
    grad_out_o[0] = acc_out
    grad_in_o[0] = acc_in

    @pl.loop(1, BRICKS)
    def _(j):
        d = lax.rem(own + j, BRICKS)
        p_copy(d).wait_send()
        w_copy(d).wait_send()

    g_copy(partner).wait_send()

    @pl.loop(1, ZS)
    def _(j):
        d = 2 * lax.rem(zi + j, ZS) + core
        g_copy(d).wait_send()
        f_copy(d).wait_send()

    @pl.loop(1, XS)
    def _(j):
        for copy in x_copies(lax.rem(xi + j, XS)):
            copy.wait_send()

    @pl.loop(1, YS)
    def _(j):
        for copy in y_copies(lax.rem(yi + j, YS)):
            copy.wait_send()


def write(pixels, grad_in, grad_out, pixels_o, grad_in_o, grad_out_o, sem):
    copies = [
        pltpu.make_async_copy(a, b, sem.at[i])
        for i, (a, b) in enumerate(
            [(pixels, pixels_o), (grad_in, grad_in_o), (grad_out, grad_out_o)]
        )
    ]
    for copy in copies:
        copy.start()
    for copy in copies:
        copy.wait()


def per_device(samples, opacity, counts, depth_order, target, weight_in, weight_out):
    in_hbm = pl.BlockSpec(memory_space=pltpu.HBM)
    vmem = pl.BlockSpec(memory_space=pltpu.VMEM)
    dma = pltpu.SemaphoreType.DMA
    shapes = (
        jax.ShapeDtypeStruct((OWN, FEAT), F32),
        jax.ShapeDtypeStruct((1, 4, HID), F32),
        jax.ShapeDtypeStruct((1, 8, FEAT), F32),
    )
    results = pl.pallas_call(
        kernel,
        out_shape=shapes,
        in_specs=[in_hbm] * 7,
        out_specs=(vmem, vmem, vmem),
        scratch_shapes=[
            pltpu.VMEM((SLOTS, RAYS, ENC), BF16),
            pltpu.VMEM((SLOTS, RAYS), F32),
            pltpu.VMEM((1, RAYS), jnp.int32),
            pltpu.VMEM((1, BRICKS), jnp.int32),
            pltpu.VMEM((OWN, FEAT), F32),
            pltpu.VMEM((ENC, HID), BF16),
            pltpu.VMEM((HID, FEAT), BF16),
            pltpu.VMEM((BRICKS, 1, RAYS), F32),
            pltpu.VMEM((RAYS, 128), F32),
            pltpu.VMEM((RAYS, 128), F32),
            pltpu.VMEM((ZS, ROWS, HID), BF16),
            pltpu.VMEM((RAYS, HID), F32),
            pltpu.VMEM((BRICKS, OWN, FEAT), F32),
            pltpu.VMEM((BRICKS, OWN, FEAT), F32),
            pltpu.VMEM((BRICKS, OWN, FEAT), F32),
            pltpu.VMEM((ZS, ENC, ROWS), BF16),
            pltpu.VMEM((ENC, HID), F32),
            pltpu.VMEM((HID, FEAT), F32),
            pltpu.VMEM((XS, 32, HID), F32),
            pltpu.VMEM((XS, 64, FEAT), F32),
            pltpu.VMEM((YS, 4, HID), F32),
            pltpu.VMEM((YS, 8, FEAT), F32),
            pltpu.VMEM((YS, 4, HID), F32),
            pltpu.VMEM((YS, 8, FEAT), F32),
            dma((6,)), dma((ZS,)),
            dma((BRICKS,)), dma((BRICKS,)),
            dma((BRICKS,)), dma((BRICKS,)),
            dma((BRICKS,)), dma((BRICKS,)),
            dma((BRICKS,)), dma((BRICKS,)),
            dma((XS, 2)), dma((XS, 2)),
            dma((YS, 2)), dma((YS, 2)),
        ],
        compiler_params=pltpu.CompilerParams(
            collective_id=0, has_side_effects=True, vmem_limit_bytes=32 * 2**20
        ),
        name="field_step",
    )(*(
        pltpu.with_memory_space_constraint(a, pltpu.HBM)
        for a in (samples, opacity, counts, depth_order, target, weight_in, weight_out)
    ))
    return pl.pallas_call(
        write,
        out_shape=shapes,
        in_specs=[vmem] * 3,
        out_specs=(in_hbm,) * 3,
        scratch_shapes=[dma((3,))],
        compiler_params=pltpu.CompilerParams(vmem_limit_bytes=2**20),
        name="write_results",
    )(*results)


def solution(mesh):
    placed = (
        P("depth", None, "tile", None),
        P("depth", None, "tile"),
        P("depth", "tile"),
        P("tile", None),
        P(("tile", "depth"), None),
        P("depth", None, None),
        P("depth", None, None),
    )
    return jax.shard_map(
        per_device,
        mesh=mesh,
        in_specs=placed,
        out_specs=(P(("tile", "depth"), None), P("depth", "tile", None), P("depth", "tile", None)),
        check_vma=False,
    )
```

```python
import jax
import jax.numpy as jnp
from jax import lax
from jax.experimental import pallas as pl
from jax.experimental.pallas import tpu as pltpu
from jax.sharding import PartitionSpec as P

ENC, HID, FEAT, SLOTS, RAYS = 128, 256, 128, 16, 512
BRICKS, OWN = 16, 32
EARLY = 3
ZS, XS, YS = 8, 4, 8
PAIR = 2 * OWN
ROWS = SLOTS * PAIR
HALF = SLOTS * OWN
MESH = pl.DeviceIdType.MESH
F32, BF16 = jnp.float32, jnp.bfloat16


def dot(a, b):
    return jnp.dot(a, b, preferred_element_type=F32)


def dot_t(a, b):
    return lax.dot_general(a, b, (((1,), (1,)), ((), ())), preferred_element_type=F32)


def split(a):
    high = a.astype(BF16)
    return high, (a - high.astype(F32)).astype(BF16)


def far_first(k):
    return lax.rem(4 + (1 - 2 * lax.rem(k, 2)) * lax.div(k + 1, 2) + 8, 8)


def kernel(
    samples_h, opacity_h, counts_h, order_h, target_h, first_h, second_h,
    pixels_o, grad_in_o, grad_out_o,
    xs, op, cnt, order, tgt, w1, w2,
    passed, near, ct, vt, vc, hid, total, sums, wsend, wrecv, pgs, fst, gin, gout,
    xin, xout, ysin, ysout, yin, yout,
    load_sem, chunk_sem, n_send, n_recv, p_send, p_recv, w_send, w_recv, g_send, g_recv, f_send, f_recv,
    x_send, x_recv, y_send, y_recv,
):
    tile = lax.axis_index("tile")
    own = lax.axis_index("depth")
    zi, core = lax.div(own, 2), lax.rem(own, 2)
    xi, yi = lax.div(tile, YS), lax.rem(tile, YS)
    partner = 2 * zi + 1 - core

    barrier = pltpu.get_barrier_semaphore()

    def greet(t, d):
        pl.semaphore_signal(
            barrier, inc=1, device_id={"tile": t, "depth": d}, device_id_type=MESH
        )

    for j in (8, 9, 7, 10, 6, 11, 5, 12, 4, 13, 3, 14, 2, 15, 1):
        greet(tile, lax.rem(own + j, BRICKS))
    for j in range(1, XS):
        greet(lax.rem(xi + j, XS) * YS + yi, own)
    for j in range(1, YS):
        greet(xi * YS + lax.rem(yi + j, YS), own)

    loads = [
        pltpu.make_async_copy(a, b, load_sem.at[i])
        for i, (a, b) in enumerate(
            [
                (opacity_h.at[0], op), (counts_h, cnt), (first_h.at[0], w1),
                (second_h.at[0], w2), (order_h, order), (target_h, tgt),
            ]
        )
    ]
    for load in loads[:3]:
        load.start()

    def rays_of(zt):
        return pl.ds(pl.multiple_of(zt * PAIR, PAIR), PAIR)

    def fetch(k):
        rays = rays_of(lax.rem(zi + far_first(k), ZS))
        return pltpu.make_async_copy(samples_h.at[0, :, rays, :], xs.at[:, rays, :], chunk_sem.at[k])

    for k in range(ZS):
        fetch(k).start()
    for load in loads[3:]:
        load.start()

    def remote(src, dst, send, recv, t, d):
        return pltpu.make_async_remote_copy(
            src_ref=src, dst_ref=dst, send_sem=send, recv_sem=recv,
            device_id={"tile": t, "depth": d}, device_id_type=MESH,
        )

    loads[0].wait()
    loads[1].wait()
    slot = lax.broadcasted_iota(jnp.int32, (SLOTS, RAYS), 0)
    living = jnp.where(slot < cnt[...], 1.0, 0.0).astype(F32)
    alpha = op[...] * living
    kept = 1.0 - alpha
    through = jnp.ones((1, RAYS), F32)
    rows = []
    for s in range(SLOTS):
        rows.append(alpha[s : s + 1] * through)
        through = through * kept[s : s + 1]
    contrib = jnp.concatenate(rows + [jnp.zeros((128 - SLOTS, RAYS), F32)], axis=0)
    for q in range(4):
        passed[own, q] = through[:, 128 * q : 128 * q + 128]
    ct[...] = contrib.T

    def n_copy(d):
        return remote(
            passed.at[own, lax.div(d, 4)], near.at[own], n_send.at[d], n_recv.at[own], tile, d
        )

    def p_copy(d):
        return remote(passed.at[own], passed.at[own], p_send.at[d], p_recv.at[own], tile, d)

    loads[2].wait()
    loads[3].wait()

    def w_copy(d):
        return remote(wsend.at[d], wrecv.at[own], w_send.at[d], w_recv.at[own], tile, d)

    def forward(zt):
        rays = rays_of(zt)
        flat = xs[:, rays, :].reshape(ROWS, ENC)
        act = jnp.maximum(dot(flat, w1[...]), 0.0)
        rounded = act.astype(BF16).reshape(SLOTS, 2, OWN, HID)
        for c in range(2):
            hid[c, zt] = rounded[:, c].reshape(HALF, HID)
        cols = ct[rays, :]
        acc = jnp.zeros((PAIR, HID), F32)
        for s in range(SLOTS):
            acc = acc + act[s * PAIR : (s + 1) * PAIR] * cols[:, s : s + 1]
        total[rays, :] = acc
        high, low = split(acc)
        term = dot(high, w2[...]) + dot(low, w2[...])
        wsend[pl.ds(2 * zt, 2)] = term.reshape(2, OWN, FEAT)

    def send_pair(zt):
        for d in (2 * zt, 2 * zt + 1):
            n_copy(d).start()
            w_copy(d).start()

    @pl.loop(0, EARLY)
    def _(k):
        fetch(k).wait()
        forward(lax.rem(zi + far_first(k), ZS))

    pl.semaphore_wait(barrier, BRICKS - 1 + XS - 1 + YS - 1)

    @pl.loop(0, EARLY)
    def _(k):
        send_pair(lax.rem(zi + far_first(k), ZS))

    @pl.loop(EARLY, ZS - 1)
    def _(k):
        zt = lax.rem(zi + far_first(k), ZS)
        fetch(k).wait()
        forward(zt)
        send_pair(zt)

    fetch(ZS - 1).wait()
    forward(zi)
    n_copy(partner).start()
    w_copy(partner).start()
    wrecv[own] = wsend[own]
    near[own] = passed[own, lax.div(own, 4)]

    @pl.loop(0, ZS - 1)
    def _(k):
        zt = lax.rem(zi + far_first(k), ZS)
        p_copy(2 * zt).start()
        p_copy(2 * zt + 1).start()

    p_copy(partner).start()

    @pl.loop(0, ZS)
    def _(zt):
        rays = rays_of(zt)
        cols = ct[rays, :]
        parts = []
        for s in range(SLOTS):
            parts.append((xs[s, rays, :].astype(F32) * cols[:, s : s + 1]).astype(BF16))
        for c in range(2):
            half = jnp.concatenate([part[c * OWN : c * OWN + OWN] for part in parts], axis=0)
            fst[c, zt] = half.T

    loads[4].wait()
    loads[5].wait()

    @pl.loop(1, BRICKS)
    def _(j):
        d = lax.rem(own + j, BRICKS)
        remote(near.at[d], near.at[d], n_send.at[d], n_recv.at[d], tile, d).wait_recv()

    rank = order[...].astype(F32)
    grid = (BRICKS, BRICKS)
    ranks = jnp.broadcast_to(rank, grid)
    row, col = (lax.broadcasted_iota(jnp.int32, grid, i) for i in range(2))
    rank_col = jnp.sum(jnp.where(row == col, ranks, 0.0), axis=1, keepdims=True)
    own_rank = jnp.sum(jnp.where(col[:1] == own, rank, 0.0), axis=1, keepdims=True)

    def product(ahead, every):
        chosen = jnp.where(rank_col < ahead, every, 1.0)
        chosen = chosen[:8] * chosen[8:]
        chosen = chosen[:4] * chosen[4:]
        chosen = chosen[:2] * chosen[2:]
        return chosen[:1] * chosen[1:]

    every = jnp.concatenate([near[b] for b in range(BRICKS)], axis=0)
    veils = [product(rank[:, b : b + 1], every) for b in range(BRICKS)]
    vt[...] = jnp.concatenate(veils + [jnp.zeros((128 - BRICKS, 128), F32)], axis=0).T

    @pl.loop(1, BRICKS)
    def _(j):
        d = lax.rem(own + j, BRICKS)
        remote(wsend.at[d], wrecv.at[d], w_send.at[d], w_recv.at[d], tile, d).wait_recv()

    mine = vt[pl.ds(pl.multiple_of(lax.rem(own, 4) * OWN, OWN), OWN), :]
    pixels = jnp.zeros((OWN, FEAT), F32)
    for b in range(BRICKS):
        pixels = pixels + wrecv[b] * mine[:, b : b + 1]
    pixels_o[...] = pixels
    pgs[own] = pixels - tgt[...]

    def g_copy(d):
        return remote(pgs.at[own], pgs.at[own], g_send.at[d], g_recv.at[own], tile, d)

    def f_copy(b):
        return remote(pgs.at[b], pgs.at[b], f_send.at[b], f_recv.at[b], tile, partner)

    @pl.loop(0, ZS - 1)
    def _(k):
        g_copy(2 * lax.rem(zi + far_first(k), ZS) + core).start()

    g_copy(partner).start()

    @pl.loop(1, BRICKS)
    def _(j):
        d = lax.rem(own + j, BRICKS)
        remote(passed.at[d], passed.at[d], p_send.at[d], p_recv.at[d], tile, d).wait_recv()

    for q in range(4):
        every = jnp.concatenate([passed[b, q] for b in range(BRICKS)], axis=0)
        veil = product(own_rank, every)
        vc[128 * q : 128 * q + 128, :] = jnp.broadcast_to(veil, (128, 128)).T

    for c in range(2):
        half = jnp.concatenate(
            [total[PAIR * z + OWN * c : PAIR * z + OWN * c + OWN, :] for z in range(ZS)], axis=0
        )
        sums[c] = half.T.astype(BF16)

    @pl.loop(1, BRICKS)
    def _(j):
        d = lax.rem(own + j, BRICKS)
        n_copy(d).wait_send()
        p_copy(d).wait_send()
        w_copy(d).wait_send()

    def wait_g(b):
        remote(pgs.at[b], pgs.at[b], g_send.at[b], g_recv.at[b], tile, b).wait_recv()

    def gradient(c):
        grads = jnp.concatenate([pgs[2 * z + c] for z in range(ZS)], axis=0)
        cols = [vc[pl.ds(pl.multiple_of(PAIR * z + OWN * c, OWN), OWN), :] for z in range(ZS)]
        high, low = split(grads * jnp.concatenate(cols, axis=0))
        return high, (dot_t(high, w2[...]) + dot_t(low, w2[...])).astype(BF16)

    def grad_in_of(c, spread):
        acc = jnp.zeros((ENC, HID), F32)
        for z in range(ZS):
            mine = spread[OWN * z : OWN * z + OWN]
            parts = []
            for s in range(SLOTS):
                live = hid[c, z, s * OWN : s * OWN + OWN, :] > 0
                parts.append(jnp.where(live, mine, jnp.zeros_like(mine)))
            acc = acc + dot(fst[c, z], jnp.concatenate(parts, axis=0))
        return acc

    for k in range(ZS - 1):
        b = 2 * lax.rem(zi + far_first(6 - k), ZS) + core
        wait_g(b)
        f_copy(b).start()

    high, spread = gradient(core)
    gout[...] = dot(sums[core], high)
    gin[...] = grad_in_of(core, spread)

    wait_g(partner)
    for k in range(ZS - 1):
        f_copy(2 * lax.rem(zi + far_first(6 - k), ZS) + 1 - core).wait_recv()

    high, spread = gradient(1 - core)
    gout[...] += dot(sums[1 - core], high)

    def x_copies(xt, which=(0, 1)):
        t = xt * YS + yi
        rin, rout = pl.ds(pl.multiple_of(32 * xt, 32), 32), pl.ds(pl.multiple_of(64 * xt, 64), 64)
        ends = ((gout.at[rout], xout.at[xi]), (gin.at[rin], xin.at[xi]))
        return [remote(*ends[i], x_send.at[xt, i], x_recv.at[xi, i], t, own) for i in which]

    def x_arrivals(xt):
        t = xt * YS + yi
        rin, rout = pl.ds(pl.multiple_of(32 * xt, 32), 32), pl.ds(pl.multiple_of(64 * xt, 64), 64)
        return (
            remote(gout.at[rout], xout.at[xt], x_send.at[xt, 0], x_recv.at[xt, 0], t, own),
            remote(gin.at[rin], xin.at[xt], x_send.at[xt, 1], x_recv.at[xt, 1], t, own),
        )

    for j in (2, 1, 3):
        x_copies(lax.rem(xi + j, XS), (0,))[0].start()
    gin[...] += grad_in_of(1 - core, spread)
    for j in (2, 1, 3):
        x_copies(lax.rem(xi + j, XS), (1,))[0].start()
    xout[xi] = gout[pl.ds(pl.multiple_of(64 * xi, 64), 64), :]
    xin[xi] = gin[pl.ds(pl.multiple_of(32 * xi, 32), 32), :]

    g_copy(partner).wait_send()

    @pl.loop(1, ZS)
    def _(j):
        d = 2 * lax.rem(zi + j, ZS) + core
        g_copy(d).wait_send()
        f_copy(d).wait_send()

    for j in (1, 3, 2):
        for copy in x_arrivals(lax.rem(xi + j, XS)):
            copy.wait_recv()
    sum_out = xout[0] + xout[1] + xout[2] + xout[3]
    sum_in = xin[0] + xin[1] + xin[2] + xin[3]
    ysout[...] = sum_out.reshape(YS, 8, FEAT)
    for j in range(YS):
        ysin[j] = sum_in[4 * j : 4 * j + 4]

    def y_copies(yt):
        t = xi * YS + yt
        return (
            remote(ysout.at[yt], yout.at[yi], y_send.at[yt, 0], y_recv.at[yi, 0], t, own),
            remote(ysin.at[yt], yin.at[yi], y_send.at[yt, 1], y_recv.at[yi, 1], t, own),
        )

    def y_arrivals(yt):
        t = xi * YS + yt
        return (
            remote(ysout.at[yt], yout.at[yt], y_send.at[yt, 0], y_recv.at[yt, 0], t, own),
            remote(ysin.at[yt], yin.at[yt], y_send.at[yt, 1], y_recv.at[yt, 1], t, own),
        )

    for j in (4, 3, 5, 2, 6, 1, 7):
        for copy in y_copies(lax.rem(yi + j, YS)):
            copy.start()

    yout[yi] = ysout[yi]
    yin[yi] = ysin[yi]

    for j in range(1, XS):
        for copy in x_copies(lax.rem(xi + j, XS)):
            copy.wait_send()

    for j in (1, 7, 2, 6, 3, 5, 4):
        for copy in y_arrivals(lax.rem(yi + j, YS)):
            copy.wait_recv()

    acc_out, acc_in = yout[0], yin[0]
    for j in range(1, YS):
        acc_out = acc_out + yout[j]
        acc_in = acc_in + yin[j]
    grad_out_o[0] = acc_out
    grad_in_o[0] = acc_in

    for j in range(1, YS):
        for copy in y_copies(lax.rem(yi + j, YS)):
            copy.wait_send()


def write(pixels, grad_in, grad_out, pixels_o, grad_in_o, grad_out_o, sem):
    copies = [
        pltpu.make_async_copy(a, b, sem.at[i])
        for i, (a, b) in enumerate(
            [(pixels, pixels_o), (grad_in, grad_in_o), (grad_out, grad_out_o)]
        )
    ]
    for copy in copies:
        copy.start()
    for copy in copies:
        copy.wait()


def per_device(samples, opacity, counts, depth_order, target, weight_in, weight_out):
    in_hbm = pl.BlockSpec(memory_space=pltpu.HBM)
    vmem = pl.BlockSpec(memory_space=pltpu.VMEM)
    dma = pltpu.SemaphoreType.DMA
    shapes = (
        jax.ShapeDtypeStruct((OWN, FEAT), F32),
        jax.ShapeDtypeStruct((1, 4, HID), F32),
        jax.ShapeDtypeStruct((1, 8, FEAT), F32),
    )
    results = pl.pallas_call(
        kernel,
        out_shape=shapes,
        in_specs=[in_hbm] * 7,
        out_specs=(vmem, vmem, vmem),
        scratch_shapes=[
            pltpu.VMEM((SLOTS, RAYS, ENC), BF16),
            pltpu.VMEM((SLOTS, RAYS), F32),
            pltpu.VMEM((1, RAYS), jnp.int32),
            pltpu.VMEM((1, BRICKS), jnp.int32),
            pltpu.VMEM((OWN, FEAT), F32),
            pltpu.VMEM((ENC, HID), BF16),
            pltpu.VMEM((HID, FEAT), BF16),
            pltpu.VMEM((BRICKS, 4, 1, 128), F32),
            pltpu.VMEM((BRICKS, 1, 128), F32),
            pltpu.VMEM((RAYS, 128), F32),
            pltpu.VMEM((128, 128), F32),
            pltpu.VMEM((RAYS, 128), F32),
            pltpu.VMEM((2, ZS, HALF, HID), BF16),
            pltpu.VMEM((RAYS, HID), F32),
            pltpu.VMEM((2, HID, RAYS // 2), BF16),
            pltpu.VMEM((BRICKS, OWN, FEAT), F32),
            pltpu.VMEM((BRICKS, OWN, FEAT), F32),
            pltpu.VMEM((BRICKS, OWN, FEAT), F32),
            pltpu.VMEM((2, ZS, ENC, HALF), BF16),
            pltpu.VMEM((ENC, HID), F32),
            pltpu.VMEM((HID, FEAT), F32),
            pltpu.VMEM((XS, 32, HID), F32),
            pltpu.VMEM((XS, 64, FEAT), F32),
            pltpu.VMEM((YS, 4, HID), F32),
            pltpu.VMEM((YS, 8, FEAT), F32),
            pltpu.VMEM((YS, 4, HID), F32),
            pltpu.VMEM((YS, 8, FEAT), F32),
            dma((6,)), dma((ZS,)),
            dma((BRICKS,)), dma((BRICKS,)),
            dma((BRICKS,)), dma((BRICKS,)),
            dma((BRICKS,)), dma((BRICKS,)),
            dma((BRICKS,)), dma((BRICKS,)),
            dma((BRICKS,)), dma((BRICKS,)),
            dma((XS, 2)), dma((XS, 2)),
            dma((YS, 2)), dma((YS, 2)),
        ],
        compiler_params=pltpu.CompilerParams(
            collective_id=0, has_side_effects=True, vmem_limit_bytes=32 * 2**20
        ),
        name="field_step",
    )(*(
        pltpu.with_memory_space_constraint(a, pltpu.HBM)
        for a in (samples, opacity, counts, depth_order, target, weight_in, weight_out)
    ))
    return pl.pallas_call(
        write,
        out_shape=shapes,
        in_specs=[vmem] * 3,
        out_specs=(in_hbm,) * 3,
        scratch_shapes=[dma((3,))],
        compiler_params=pltpu.CompilerParams(vmem_limit_bytes=2**20),
        name="write_results",
    )(*results)


def solution(mesh):
    placed = (
        P("depth", None, "tile", None),
        P("depth", None, "tile"),
        P("depth", "tile"),
        P("tile", None),
        P(("tile", "depth"), None),
        P("depth", None, None),
        P("depth", None, None),
    )
    return jax.shard_map(
        per_device,
        mesh=mesh,
        in_specs=placed,
        out_specs=(P(("tile", "depth"), None), P("depth", "tile", None), P("depth", "tile", None)),
        check_vma=False,
    )
```

```python
import jax
import jax.numpy as jnp
from jax import lax
from jax.experimental import pallas as pl
from jax.experimental.pallas import tpu as pltpu
from jax.sharding import PartitionSpec as P

ENC, HID, FEAT, SLOTS, RAYS = 128, 256, 128, 16, 512
BRICKS, OWN = 16, 32
EARLY = 3
ZS, XS, YS = 8, 4, 8
PAIR = 2 * OWN
ROWS = SLOTS * PAIR
HALF = SLOTS * OWN
MESH = pl.DeviceIdType.MESH
F32, BF16 = jnp.float32, jnp.bfloat16


def dot(a, b):
    return jnp.dot(a, b, preferred_element_type=F32)


def dot_t(a, b):
    return lax.dot_general(a, b, (((1,), (1,)), ((), ())), preferred_element_type=F32)


def split(a):
    high = a.astype(BF16)
    return high, (a - high.astype(F32)).astype(BF16)


def far_first(k):
    return lax.rem(4 + (1 - 2 * lax.rem(k, 2)) * lax.div(k + 1, 2) + 8, 8)


def kernel(
    samples_h, opacity_h, counts_h, order_h, target_h, first_h, second_h,
    pixels_o, grad_in_o, grad_out_o,
    xs, op, cnt, order, tgt, w1, w2,
    passed, near, ct, vt, vc, hid, total, sums, wsend, wrecv, pgs, fst, gin, gout,
    xin, xout, ysin, ysout, yin, yout,
    load_sem, chunk_sem, n_send, n_recv, p_send, p_recv, w_send, w_recv, g_send, g_recv, f_send, f_recv,
    x_send, x_recv, y_send, y_recv,
):
    tile = lax.axis_index("tile")
    own = lax.axis_index("depth")
    zi, core = lax.div(own, 2), lax.rem(own, 2)
    xi, yi = lax.div(tile, YS), lax.rem(tile, YS)
    partner = 2 * zi + 1 - core

    barrier = pltpu.get_barrier_semaphore()

    def greet(t, d):
        pl.semaphore_signal(
            barrier, inc=1, device_id={"tile": t, "depth": d}, device_id_type=MESH
        )

    for j in (8, 9, 7, 10, 6, 11, 5, 12, 4, 13, 3, 14, 2, 15, 1):
        greet(tile, lax.rem(own + j, BRICKS))
    for j in range(1, XS):
        greet(lax.rem(xi + j, XS) * YS + yi, own)
    for j in range(1, YS):
        greet(xi * YS + lax.rem(yi + j, YS), own)

    loads = [
        pltpu.make_async_copy(a, b, load_sem.at[i])
        for i, (a, b) in enumerate(
            [
                (opacity_h.at[0], op), (counts_h, cnt), (first_h.at[0], w1),
                (second_h.at[0], w2), (order_h, order), (target_h, tgt),
            ]
        )
    ]
    for load in loads[:3]:
        load.start()

    def rays_of(zt):
        return pl.ds(pl.multiple_of(zt * PAIR, PAIR), PAIR)

    def fetch(k):
        rays = rays_of(lax.rem(zi + far_first(k), ZS))
        return pltpu.make_async_copy(samples_h.at[0, :, rays, :], xs.at[:, rays, :], chunk_sem.at[k])

    for k in range(ZS):
        fetch(k).start()
    for load in loads[3:]:
        load.start()

    def remote(src, dst, send, recv, t, d):
        return pltpu.make_async_remote_copy(
            src_ref=src, dst_ref=dst, send_sem=send, recv_sem=recv,
            device_id={"tile": t, "depth": d}, device_id_type=MESH,
        )

    loads[0].wait()
    loads[1].wait()
    slot = lax.broadcasted_iota(jnp.int32, (SLOTS, RAYS), 0)
    living = jnp.where(slot < cnt[...], 1.0, 0.0).astype(F32)
    alpha = op[...] * living
    kept = 1.0 - alpha
    through = jnp.ones((1, RAYS), F32)
    rows = []
    for s in range(SLOTS):
        rows.append(alpha[s : s + 1] * through)
        through = through * kept[s : s + 1]
    contrib = jnp.concatenate(rows + [jnp.zeros((128 - SLOTS, RAYS), F32)], axis=0)
    for q in range(4):
        passed[own, q] = through[:, 128 * q : 128 * q + 128]
    ct[...] = contrib.T

    def all_of(ref, count, sem):
        part = ref.at[pl.ds(0, count)]
        pltpu.make_async_copy(part, part, sem).wait()

    def n_copy(d):
        return remote(
            passed.at[own, lax.div(d, 4)], near.at[own], n_send, n_recv, tile, d
        )

    def p_copy(d):
        return remote(passed.at[own], passed.at[own], p_send, p_recv, tile, d)

    loads[2].wait()
    loads[3].wait()

    def w_copy(d):
        return remote(wsend.at[d], wrecv.at[own], w_send, w_recv, tile, d)

    def forward(zt):
        rays = rays_of(zt)
        flat = xs[:, rays, :].reshape(ROWS, ENC)
        act = jnp.maximum(dot(flat, w1[...]), 0.0)
        rounded = act.astype(BF16).reshape(SLOTS, 2, OWN, HID)
        for c in range(2):
            hid[c, zt] = rounded[:, c].reshape(HALF, HID)
        cols = ct[rays, :]
        acc = jnp.zeros((PAIR, HID), F32)
        for s in range(SLOTS):
            acc = acc + act[s * PAIR : (s + 1) * PAIR] * cols[:, s : s + 1]
        total[rays, :] = acc
        high, low = split(acc)
        term = dot(high, w2[...]) + dot(low, w2[...])
        wsend[pl.ds(2 * zt, 2)] = term.reshape(2, OWN, FEAT)

    def send_pair(zt):
        w_copy(2 * zt).start()
        w_copy(2 * zt + 1).start()

    @pl.loop(0, EARLY)
    def _(k):
        fetch(k).wait()
        forward(lax.rem(zi + far_first(k), ZS))

    pl.semaphore_wait(barrier, BRICKS - 1 + XS - 1 + YS - 1)

    for j in (8, 9, 7, 10, 6, 11, 5, 12, 4, 13, 3, 14, 2, 15, 1):
        n_copy(lax.rem(own + j, BRICKS)).start()

    @pl.loop(0, EARLY)
    def _(k):
        send_pair(lax.rem(zi + far_first(k), ZS))

    @pl.loop(EARLY, ZS - 1)
    def _(k):
        zt = lax.rem(zi + far_first(k), ZS)
        fetch(k).wait()
        forward(zt)
        send_pair(zt)

    fetch(ZS - 1).wait()
    forward(zi)
    w_copy(partner).start()
    wrecv[own] = wsend[own]
    near[own] = passed[own, lax.div(own, 4)]

    @pl.loop(0, ZS - 1)
    def _(k):
        zt = lax.rem(zi + far_first(k), ZS)
        p_copy(2 * zt).start()
        p_copy(2 * zt + 1).start()

    p_copy(partner).start()

    @pl.loop(0, ZS)
    def _(zt):
        rays = rays_of(zt)
        cols = ct[rays, :]
        parts = []
        for s in range(SLOTS):
            parts.append((xs[s, rays, :].astype(F32) * cols[:, s : s + 1]).astype(BF16))
        for c in range(2):
            half = jnp.concatenate([part[c * OWN : c * OWN + OWN] for part in parts], axis=0)
            fst[c, zt] = half.T

    loads[4].wait()
    loads[5].wait()

    all_of(near, BRICKS - 1, n_recv)

    rank = order[...].astype(F32)
    grid = (BRICKS, BRICKS)
    ranks = jnp.broadcast_to(rank, grid)
    row, col = (lax.broadcasted_iota(jnp.int32, grid, i) for i in range(2))
    rank_col = jnp.sum(jnp.where(row == col, ranks, 0.0), axis=1, keepdims=True)
    own_rank = jnp.sum(jnp.where(col[:1] == own, rank, 0.0), axis=1, keepdims=True)

    def product(ahead, every):
        chosen = jnp.where(rank_col < ahead, every, 1.0)
        chosen = chosen[:8] * chosen[8:]
        chosen = chosen[:4] * chosen[4:]
        chosen = chosen[:2] * chosen[2:]
        return chosen[:1] * chosen[1:]

    every = jnp.concatenate([near[b] for b in range(BRICKS)], axis=0)
    veils = [product(rank[:, b : b + 1], every) for b in range(BRICKS)]
    vt[...] = jnp.concatenate(veils + [jnp.zeros((128 - BRICKS, 128), F32)], axis=0).T

    all_of(wrecv, BRICKS - 1, w_recv)

    mine = vt[pl.ds(pl.multiple_of(lax.rem(own, 4) * OWN, OWN), OWN), :]
    pixels = jnp.zeros((OWN, FEAT), F32)
    for b in range(BRICKS):
        pixels = pixels + wrecv[b] * mine[:, b : b + 1]
    pixels_o[...] = pixels
    pgs[own] = pixels - tgt[...]

    def g_copy(d):
        return remote(pgs.at[own], pgs.at[own], g_send, g_recv.at[zi], tile, d)

    def f_copy(b):
        return remote(pgs.at[b], pgs.at[b], f_send, f_recv, tile, partner)

    @pl.loop(0, ZS - 1)
    def _(k):
        g_copy(2 * lax.rem(zi + far_first(k), ZS) + core).start()

    g_copy(partner).start()

    all_of(passed, BRICKS - 1, p_recv)

    for q in range(4):
        every = jnp.concatenate([passed[b, q] for b in range(BRICKS)], axis=0)
        veil = product(own_rank, every)
        vc[128 * q : 128 * q + 128, :] = jnp.broadcast_to(veil, (128, 128)).T

    for c in range(2):
        half = jnp.concatenate(
            [total[PAIR * z + OWN * c : PAIR * z + OWN * c + OWN, :] for z in range(ZS)], axis=0
        )
        sums[c] = half.T.astype(BF16)

    all_of(near, BRICKS - 1, n_send)
    all_of(passed, BRICKS - 1, p_send)
    all_of(wsend, BRICKS - 1, w_send)

    def wait_g(b):
        pltpu.make_async_copy(pgs.at[b], pgs.at[b], g_recv.at[lax.div(b, 2)]).wait()

    def gradient(c):
        grads = jnp.concatenate([pgs[2 * z + c] for z in range(ZS)], axis=0)
        cols = [vc[pl.ds(pl.multiple_of(PAIR * z + OWN * c, OWN), OWN), :] for z in range(ZS)]
        high, low = split(grads * jnp.concatenate(cols, axis=0))
        return high, (dot_t(high, w2[...]) + dot_t(low, w2[...])).astype(BF16)

    def grad_in_of(c, spread):
        acc = jnp.zeros((ENC, HID), F32)
        for z in range(ZS):
            mine = spread[OWN * z : OWN * z + OWN]
            parts = []
            for s in range(SLOTS):
                live = hid[c, z, s * OWN : s * OWN + OWN, :] > 0
                parts.append(jnp.where(live, mine, jnp.zeros_like(mine)))
            acc = acc + dot(fst[c, z], jnp.concatenate(parts, axis=0))
        return acc

    for k in range(ZS - 1):
        b = 2 * lax.rem(zi + far_first(6 - k), ZS) + core
        wait_g(b)
        f_copy(b).start()

    high, spread = gradient(core)
    gout[...] = dot(sums[core], high)
    gin[...] = grad_in_of(core, spread)

    wait_g(partner)
    all_of(pgs, ZS - 1, f_recv)

    high, spread = gradient(1 - core)
    gout[...] += dot(sums[1 - core], high)

    def x_copies(xt, which):
        t = xt * YS + yi
        rin, rout = pl.ds(pl.multiple_of(32 * xt, 32), 32), pl.ds(pl.multiple_of(64 * xt, 64), 64)
        src, dst = ((gout.at[rout], xout.at[xi]), (gin.at[rin], xin.at[xi]))[which]
        return remote(src, dst, x_send.at[which], x_recv.at[which], t, own)

    for j in (2, 1, 3):
        x_copies(lax.rem(xi + j, XS), 0).start()
    gin[...] += grad_in_of(1 - core, spread)
    for j in (2, 1, 3):
        x_copies(lax.rem(xi + j, XS), 1).start()
    xout[xi] = gout[pl.ds(pl.multiple_of(64 * xi, 64), 64), :]
    xin[xi] = gin[pl.ds(pl.multiple_of(32 * xi, 32), 32), :]

    all_of(pgs, ZS, g_send)
    all_of(pgs, ZS - 1, f_send)

    all_of(xout, XS - 1, x_recv.at[0])
    all_of(xin, XS - 1, x_recv.at[1])
    sum_out = xout[0] + xout[1] + xout[2] + xout[3]
    sum_in = xin[0] + xin[1] + xin[2] + xin[3]
    ysout[...] = sum_out.reshape(YS, 8, FEAT)
    for j in range(YS):
        ysin[j] = sum_in[4 * j : 4 * j + 4]

    def y_copies(yt):
        t = xi * YS + yt
        return (
            remote(ysout.at[yt], yout.at[yi], y_send.at[0], y_recv.at[0], t, own),
            remote(ysin.at[yt], yin.at[yi], y_send.at[1], y_recv.at[1], t, own),
        )

    for j in (4, 3, 5, 2, 6, 1, 7):
        for copy in y_copies(lax.rem(yi + j, YS)):
            copy.start()

    yout[yi] = ysout[yi]
    yin[yi] = ysin[yi]

    all_of(xout, XS - 1, x_send.at[0])
    all_of(xin, XS - 1, x_send.at[1])
    all_of(yout, YS - 1, y_recv.at[0])
    all_of(yin, YS - 1, y_recv.at[1])

    acc_out, acc_in = yout[0], yin[0]
    for j in range(1, YS):
        acc_out = acc_out + yout[j]
        acc_in = acc_in + yin[j]
    grad_out_o[0] = acc_out
    grad_in_o[0] = acc_in

    all_of(yout, YS - 1, y_send.at[0])
    all_of(yin, YS - 1, y_send.at[1])


def write(pixels, grad_in, grad_out, pixels_o, grad_in_o, grad_out_o, sem):
    copies = [
        pltpu.make_async_copy(a, b, sem.at[i])
        for i, (a, b) in enumerate(
            [(pixels, pixels_o), (grad_in, grad_in_o), (grad_out, grad_out_o)]
        )
    ]
    for copy in copies:
        copy.start()
    for copy in copies:
        copy.wait()


def per_device(samples, opacity, counts, depth_order, target, weight_in, weight_out):
    in_hbm = pl.BlockSpec(memory_space=pltpu.HBM)
    vmem = pl.BlockSpec(memory_space=pltpu.VMEM)
    dma = pltpu.SemaphoreType.DMA
    shapes = (
        jax.ShapeDtypeStruct((OWN, FEAT), F32),
        jax.ShapeDtypeStruct((1, 4, HID), F32),
        jax.ShapeDtypeStruct((1, 8, FEAT), F32),
    )
    results = pl.pallas_call(
        kernel,
        out_shape=shapes,
        in_specs=[in_hbm] * 7,
        out_specs=(vmem, vmem, vmem),
        scratch_shapes=[
            pltpu.VMEM((SLOTS, RAYS, ENC), BF16),
            pltpu.VMEM((SLOTS, RAYS), F32),
            pltpu.VMEM((1, RAYS), jnp.int32),
            pltpu.VMEM((1, BRICKS), jnp.int32),
            pltpu.VMEM((OWN, FEAT), F32),
            pltpu.VMEM((ENC, HID), BF16),
            pltpu.VMEM((HID, FEAT), BF16),
            pltpu.VMEM((BRICKS, 4, 1, 128), F32),
            pltpu.VMEM((BRICKS, 1, 128), F32),
            pltpu.VMEM((RAYS, 128), F32),
            pltpu.VMEM((128, 128), F32),
            pltpu.VMEM((RAYS, 128), F32),
            pltpu.VMEM((2, ZS, HALF, HID), BF16),
            pltpu.VMEM((RAYS, HID), F32),
            pltpu.VMEM((2, HID, RAYS // 2), BF16),
            pltpu.VMEM((BRICKS, OWN, FEAT), F32),
            pltpu.VMEM((BRICKS, OWN, FEAT), F32),
            pltpu.VMEM((BRICKS, OWN, FEAT), F32),
            pltpu.VMEM((2, ZS, ENC, HALF), BF16),
            pltpu.VMEM((ENC, HID), F32),
            pltpu.VMEM((HID, FEAT), F32),
            pltpu.VMEM((XS, 32, HID), F32),
            pltpu.VMEM((XS, 64, FEAT), F32),
            pltpu.VMEM((YS, 4, HID), F32),
            pltpu.VMEM((YS, 8, FEAT), F32),
            pltpu.VMEM((YS, 4, HID), F32),
            pltpu.VMEM((YS, 8, FEAT), F32),
            dma((6,)), dma((ZS,)),
            dma(()), dma(()), dma(()), dma(()), dma(()), dma(()),
            dma(()), dma((ZS,)), dma(()), dma(()),
            dma((2,)), dma((2,)), dma((2,)), dma((2,)),
        ],
        compiler_params=pltpu.CompilerParams(
            collective_id=0, has_side_effects=True, vmem_limit_bytes=32 * 2**20
        ),
        name="field_step",
    )(*(
        pltpu.with_memory_space_constraint(a, pltpu.HBM)
        for a in (samples, opacity, counts, depth_order, target, weight_in, weight_out)
    ))
    return pl.pallas_call(
        write,
        out_shape=shapes,
        in_specs=[vmem] * 3,
        out_specs=(in_hbm,) * 3,
        scratch_shapes=[dma((3,))],
        compiler_params=pltpu.CompilerParams(vmem_limit_bytes=2**20),
        name="write_results",
    )(*results)


def solution(mesh):
    placed = (
        P("depth", None, "tile", None),
        P("depth", None, "tile"),
        P("depth", "tile"),
        P("tile", None),
        P(("tile", "depth"), None),
        P("depth", None, None),
        P("depth", None, None),
    )
    return jax.shard_map(
        per_device,
        mesh=mesh,
        in_specs=placed,
        out_specs=(P(("tile", "depth"), None), P("depth", "tile", None), P("depth", "tile", None)),
        check_vma=False,
    )
```

```python
import jax
import jax.numpy as jnp
from jax import lax
from jax.experimental import pallas as pl
from jax.experimental.pallas import tpu as pltpu
from jax.sharding import PartitionSpec as P

ENC, HID, FEAT, SLOTS, RAYS = 128, 256, 128, 16, 512
BRICKS, OWN = 16, 32
EARLY = 3
ZS, XS, YS = 8, 4, 8
TILES = XS * YS
FAR_TILES = sorted(
    [(x, y) for x in range(XS) for y in range(YS) if x + y],
    key=lambda d: -min(d[0], XS - d[0]) - min(d[1], YS - d[1]),
)
PAIR = 2 * OWN
ROWS = SLOTS * PAIR
HALF = SLOTS * OWN
MESH = pl.DeviceIdType.MESH
F32, BF16 = jnp.float32, jnp.bfloat16


def dot(a, b):
    return jnp.dot(a, b, preferred_element_type=F32)


def dot_t(a, b):
    return lax.dot_general(a, b, (((1,), (1,)), ((), ())), preferred_element_type=F32)


def split(a):
    high = a.astype(BF16)
    return high, (a - high.astype(F32)).astype(BF16)


def far_first(k):
    return lax.rem(4 + (1 - 2 * lax.rem(k, 2)) * lax.div(k + 1, 2) + 8, 8)


def kernel(
    samples_h, opacity_h, counts_h, order_h, target_h, first_h, second_h,
    pixels_o, grad_in_o, grad_out_o,
    xs, op, cnt, order, tgt, w1, w2,
    passed, near, ct, vt, vc, hid, total, sums, wsend, wrecv, pgs, fst, gin, gout,
    grads, shares,
    load_sem, chunk_sem, n_send, n_recv, p_send, p_recv, w_send, w_recv, g_send, g_recv, f_send, f_recv,
    e_send, e_recv, met,
):
    tile = lax.axis_index("tile")
    own = lax.axis_index("depth")
    zi, core = lax.div(own, 2), lax.rem(own, 2)
    xi, yi = lax.div(tile, YS), lax.rem(tile, YS)
    partner = 2 * zi + 1 - core

    barrier = pltpu.get_barrier_semaphore()

    def greet(t, d):
        pl.semaphore_signal(
            barrier, inc=1, device_id={"tile": t, "depth": d}, device_id_type=MESH
        )

    for j in (8, 9, 7, 10, 6, 11, 5, 12, 4, 13, 3, 14, 2, 15, 1):
        greet(tile, lax.rem(own + j, BRICKS))
    for j in range(1, XS):
        greet(lax.rem(xi + j, XS) * YS + yi, own)
    for j in range(1, YS):
        greet(xi * YS + lax.rem(yi + j, YS), own)

    loads = [
        pltpu.make_async_copy(a, b, load_sem.at[i])
        for i, (a, b) in enumerate(
            [
                (opacity_h.at[0], op), (counts_h, cnt), (first_h.at[0], w1),
                (second_h.at[0], w2), (order_h, order), (target_h, tgt),
            ]
        )
    ]
    for load in loads[:3]:
        load.start()

    def rays_of(zt):
        return pl.ds(pl.multiple_of(zt * PAIR, PAIR), PAIR)

    def fetch(k):
        rays = rays_of(lax.rem(zi + far_first(k), ZS))
        return pltpu.make_async_copy(samples_h.at[0, :, rays, :], xs.at[:, rays, :], chunk_sem.at[k])

    for k in range(ZS):
        fetch(k).start()
    for load in loads[3:]:
        load.start()

    def remote(src, dst, send, recv, t, d):
        return pltpu.make_async_remote_copy(
            src_ref=src, dst_ref=dst, send_sem=send, recv_sem=recv,
            device_id={"tile": t, "depth": d}, device_id_type=MESH,
        )

    loads[0].wait()
    loads[1].wait()
    slot = lax.broadcasted_iota(jnp.int32, (SLOTS, RAYS), 0)
    living = jnp.where(slot < cnt[...], 1.0, 0.0).astype(F32)
    alpha = op[...] * living
    kept = 1.0 - alpha
    through = jnp.ones((1, RAYS), F32)
    rows = []
    for s in range(SLOTS):
        rows.append(alpha[s : s + 1] * through)
        through = through * kept[s : s + 1]
    contrib = jnp.concatenate(rows + [jnp.zeros((128 - SLOTS, RAYS), F32)], axis=0)
    for q in range(4):
        passed[own, q] = through[:, 128 * q : 128 * q + 128]
    ct[...] = contrib.T

    def all_of(ref, count, sem):
        part = ref.at[pl.ds(0, count)]
        pltpu.make_async_copy(part, part, sem).wait()

    def n_copy(d):
        return remote(
            passed.at[own, lax.div(d, 4)], near.at[own], n_send, n_recv, tile, d
        )

    def p_copy(d):
        return remote(passed.at[own], passed.at[own], p_send, p_recv, tile, d)

    loads[2].wait()
    loads[3].wait()

    def w_copy(d):
        return remote(wsend.at[d], wrecv.at[own], w_send, w_recv, tile, d)

    def forward(zt):
        rays = rays_of(zt)
        flat = xs[:, rays, :].reshape(ROWS, ENC)
        act = jnp.maximum(dot(flat, w1[...]), 0.0)
        rounded = act.astype(BF16).reshape(SLOTS, 2, OWN, HID)
        for c in range(2):
            hid[c, zt] = rounded[:, c].reshape(HALF, HID)
        cols = ct[rays, :]
        acc = jnp.zeros((PAIR, HID), F32)
        for s in range(SLOTS):
            acc = acc + act[s * PAIR : (s + 1) * PAIR] * cols[:, s : s + 1]
        total[rays, :] = acc
        high, low = split(acc)
        term = dot(high, w2[...]) + dot(low, w2[...])
        wsend[pl.ds(2 * zt, 2)] = term.reshape(2, OWN, FEAT)

    def send_pair(zt):
        w_copy(2 * zt).start()
        w_copy(2 * zt + 1).start()

    @pl.loop(0, EARLY)
    def _(k):
        fetch(k).wait()
        forward(lax.rem(zi + far_first(k), ZS))

    pl.semaphore_wait(barrier, BRICKS - 1 + XS - 1 + YS - 1)

    for j in (8, 9, 7, 10, 6, 11, 5, 12, 4, 13, 3, 14, 2, 15, 1):
        n_copy(lax.rem(own + j, BRICKS)).start()

    @pl.loop(0, EARLY)
    def _(k):
        send_pair(lax.rem(zi + far_first(k), ZS))

    @pl.loop(EARLY, ZS - 1)
    def _(k):
        zt = lax.rem(zi + far_first(k), ZS)
        fetch(k).wait()
        forward(zt)
        send_pair(zt)

    fetch(ZS - 1).wait()
    forward(zi)
    w_copy(partner).start()
    wrecv[own] = wsend[own]
    near[own] = passed[own, lax.div(own, 4)]

    for j in range(1, XS):
        pl.semaphore_signal(
            met, inc=1,
            device_id={"tile": lax.rem(xi + j, XS) * YS + yi, "depth": own},
            device_id_type=MESH,
        )

    @pl.loop(0, ZS - 1)
    def _(k):
        zt = lax.rem(zi + far_first(k), ZS)
        p_copy(2 * zt).start()
        p_copy(2 * zt + 1).start()

    p_copy(partner).start()

    @pl.loop(0, ZS)
    def _(zt):
        rays = rays_of(zt)
        cols = ct[rays, :]
        parts = []
        for s in range(SLOTS):
            parts.append((xs[s, rays, :].astype(F32) * cols[:, s : s + 1]).astype(BF16))
        for c in range(2):
            half = jnp.concatenate([part[c * OWN : c * OWN + OWN] for part in parts], axis=0)
            fst[c, zt] = half.T

    loads[4].wait()
    loads[5].wait()

    all_of(near, BRICKS - 1, n_recv)

    rank = order[...].astype(F32)
    grid = (BRICKS, BRICKS)
    ranks = jnp.broadcast_to(rank, grid)
    row, col = (lax.broadcasted_iota(jnp.int32, grid, i) for i in range(2))
    rank_col = jnp.sum(jnp.where(row == col, ranks, 0.0), axis=1, keepdims=True)
    own_rank = jnp.sum(jnp.where(col[:1] == own, rank, 0.0), axis=1, keepdims=True)

    def product(ahead, every):
        chosen = jnp.where(rank_col < ahead, every, 1.0)
        chosen = chosen[:8] * chosen[8:]
        chosen = chosen[:4] * chosen[4:]
        chosen = chosen[:2] * chosen[2:]
        return chosen[:1] * chosen[1:]

    every = jnp.concatenate([near[b] for b in range(BRICKS)], axis=0)
    veils = [product(rank[:, b : b + 1], every) for b in range(BRICKS)]
    vt[...] = jnp.concatenate(veils + [jnp.zeros((128 - BRICKS, 128), F32)], axis=0).T

    all_of(wrecv, BRICKS - 1, w_recv)

    mine = vt[pl.ds(pl.multiple_of(lax.rem(own, 4) * OWN, OWN), OWN), :]
    pixels = jnp.zeros((OWN, FEAT), F32)
    for b in range(BRICKS):
        pixels = pixels + wrecv[b] * mine[:, b : b + 1]
    pixels_o[...] = pixels
    pgs[own] = pixels - tgt[...]

    def g_copy(d):
        return remote(pgs.at[own], pgs.at[own], g_send, g_recv.at[zi], tile, d)

    def f_copy(b):
        return remote(pgs.at[b], pgs.at[b], f_send, f_recv, tile, partner)

    @pl.loop(0, ZS - 1)
    def _(k):
        g_copy(2 * lax.rem(zi + far_first(k), ZS) + core).start()

    g_copy(partner).start()

    all_of(passed, BRICKS - 1, p_recv)

    for q in range(4):
        every = jnp.concatenate([passed[b, q] for b in range(BRICKS)], axis=0)
        veil = product(own_rank, every)
        vc[128 * q : 128 * q + 128, :] = jnp.broadcast_to(veil, (128, 128)).T

    for c in range(2):
        half = jnp.concatenate(
            [total[PAIR * z + OWN * c : PAIR * z + OWN * c + OWN, :] for z in range(ZS)], axis=0
        )
        sums[c] = half.T.astype(BF16)

    all_of(near, BRICKS - 1, n_send)
    all_of(passed, BRICKS - 1, p_send)
    all_of(wsend, BRICKS - 1, w_send)

    def wait_g(b):
        pltpu.make_async_copy(pgs.at[b], pgs.at[b], g_recv.at[lax.div(b, 2)]).wait()

    def gradient(c):
        grads = jnp.concatenate([pgs[2 * z + c] for z in range(ZS)], axis=0)
        cols = [vc[pl.ds(pl.multiple_of(PAIR * z + OWN * c, OWN), OWN), :] for z in range(ZS)]
        high, low = split(grads * jnp.concatenate(cols, axis=0))
        return high, (dot_t(high, w2[...]) + dot_t(low, w2[...])).astype(BF16)

    def grad_in_of(c, spread):
        acc = jnp.zeros((ENC, HID), F32)
        for z in range(ZS):
            mine = spread[OWN * z : OWN * z + OWN]
            parts = []
            for s in range(SLOTS):
                live = hid[c, z, s * OWN : s * OWN + OWN, :] > 0
                parts.append(jnp.where(live, mine, jnp.zeros_like(mine)))
            acc = acc + dot(fst[c, z], jnp.concatenate(parts, axis=0))
        return acc

    for k in range(ZS - 1):
        b = 2 * lax.rem(zi + far_first(6 - k), ZS) + core
        wait_g(b)
        f_copy(b).start()

    high, spread = gradient(core)
    gout[...] = dot(sums[core], high)
    gin[...] = grad_in_of(core, spread)

    wait_g(partner)
    all_of(pgs, ZS - 1, f_recv)

    high, spread = gradient(1 - core)
    gout_total = gout[...] + dot(sums[1 - core], high)

    def tile_at(dx, dy):
        return lax.rem(xi + dx, XS) * YS + lax.rem(yi + dy, YS)

    def e_copy(i, t):
        return remote(grads.at[i, t], shares.at[i, tile], e_send.at[i], e_recv.at[i], t, own)

    def scatter(i):
        for dx, dy in FAR_TILES:
            e_copy(i, tile_at(dx, dy)).start()

    grads[0] = gout_total.reshape(TILES, 8, FEAT)
    pl.semaphore_wait(met, XS - 1)
    scatter(0)
    total_in = gin[...] + grad_in_of(1 - core, spread)
    for t in range(TILES):
        rows = total_in[4 * t : 4 * t + 4]
        grads[1, t] = jnp.concatenate([rows[:, :128], rows[:, 128:]], axis=0)
    scatter(1)
    for i in range(2):
        shares[i, tile] = grads[i, tile]
    all_of(pgs, ZS, g_send)
    all_of(pgs, ZS - 1, f_send)
    for i in range(2):
        all_of(shares.at[i], TILES - 1, e_recv.at[i])
    acc_out, acc_in = shares[0, 0], shares[1, 0]
    for t in range(1, TILES):
        acc_out = acc_out + shares[0, t]
        acc_in = acc_in + shares[1, t]
    grad_out_o[0] = acc_out
    grad_in_o[0] = jnp.concatenate([acc_in[:4], acc_in[4:]], axis=1)
    for i in range(2):
        all_of(grads.at[i], TILES - 1, e_send.at[i])


def write(pixels, grad_in, grad_out, pixels_o, grad_in_o, grad_out_o, sem):
    copies = [
        pltpu.make_async_copy(a, b, sem.at[i])
        for i, (a, b) in enumerate(
            [(pixels, pixels_o), (grad_in, grad_in_o), (grad_out, grad_out_o)]
        )
    ]
    for copy in copies:
        copy.start()
    for copy in copies:
        copy.wait()


def per_device(samples, opacity, counts, depth_order, target, weight_in, weight_out):
    in_hbm = pl.BlockSpec(memory_space=pltpu.HBM)
    vmem = pl.BlockSpec(memory_space=pltpu.VMEM)
    dma = pltpu.SemaphoreType.DMA
    shapes = (
        jax.ShapeDtypeStruct((OWN, FEAT), F32),
        jax.ShapeDtypeStruct((1, 4, HID), F32),
        jax.ShapeDtypeStruct((1, 8, FEAT), F32),
    )
    results = pl.pallas_call(
        kernel,
        out_shape=shapes,
        in_specs=[in_hbm] * 7,
        out_specs=(vmem, vmem, vmem),
        scratch_shapes=[
            pltpu.VMEM((SLOTS, RAYS, ENC), BF16),
            pltpu.VMEM((SLOTS, RAYS), F32),
            pltpu.VMEM((1, RAYS), jnp.int32),
            pltpu.VMEM((1, BRICKS), jnp.int32),
            pltpu.VMEM((OWN, FEAT), F32),
            pltpu.VMEM((ENC, HID), BF16),
            pltpu.VMEM((HID, FEAT), BF16),
            pltpu.VMEM((BRICKS, 4, 1, 128), F32),
            pltpu.VMEM((BRICKS, 1, 128), F32),
            pltpu.VMEM((RAYS, 128), F32),
            pltpu.VMEM((128, 128), F32),
            pltpu.VMEM((RAYS, 128), F32),
            pltpu.VMEM((2, ZS, HALF, HID), BF16),
            pltpu.VMEM((RAYS, HID), F32),
            pltpu.VMEM((2, HID, RAYS // 2), BF16),
            pltpu.VMEM((BRICKS, OWN, FEAT), F32),
            pltpu.VMEM((BRICKS, OWN, FEAT), F32),
            pltpu.VMEM((BRICKS, OWN, FEAT), F32),
            pltpu.VMEM((2, ZS, ENC, HALF), BF16),
            pltpu.VMEM((ENC, HID), F32),
            pltpu.VMEM((HID, FEAT), F32),
            pltpu.VMEM((2, TILES, 8, 128), F32),
            pltpu.VMEM((2, TILES, 8, 128), F32),
            dma((6,)), dma((ZS,)),
            dma(()), dma(()), dma(()), dma(()), dma(()), dma(()),
            dma(()), dma((ZS,)), dma(()), dma(()),
            dma((2,)), dma((2,)), pltpu.SemaphoreType.REGULAR,
        ],
        compiler_params=pltpu.CompilerParams(
            collective_id=0, has_side_effects=True, vmem_limit_bytes=32 * 2**20
        ),
        name="field_step",
    )(*(
        pltpu.with_memory_space_constraint(a, pltpu.HBM)
        for a in (samples, opacity, counts, depth_order, target, weight_in, weight_out)
    ))
    return pl.pallas_call(
        write,
        out_shape=shapes,
        in_specs=[vmem] * 3,
        out_specs=(in_hbm,) * 3,
        scratch_shapes=[dma((3,))],
        compiler_params=pltpu.CompilerParams(vmem_limit_bytes=2**20),
        name="write_results",
    )(*results)


def solution(mesh):
    placed = (
        P("depth", None, "tile", None),
        P("depth", None, "tile"),
        P("depth", "tile"),
        P("tile", None),
        P(("tile", "depth"), None),
        P("depth", None, None),
        P("depth", None, None),
    )
    return jax.shard_map(
        per_device,
        mesh=mesh,
        in_specs=placed,
        out_specs=(P(("tile", "depth"), None), P("depth", "tile", None), P("depth", "tile", None)),
        check_vma=False,
    )
```

```python
import jax
import jax.numpy as jnp
from jax import lax
from jax.experimental import pallas as pl
from jax.experimental.pallas import tpu as pltpu
from jax.sharding import PartitionSpec as P

ENC, HID, FEAT, SLOTS, RAYS = 128, 256, 128, 16, 512
BRICKS, OWN = 16, 32
EARLY = 2
FAR = (4, 3, 5, 2, 6, 1, 7, 0)
ZS, XS, YS = 8, 4, 8
TILES = XS * YS
FAR_TILES = sorted(
    [(x, y) for x in range(XS) for y in range(YS) if x + y],
    key=lambda d: -min(d[0], XS - d[0]) - min(d[1], YS - d[1]),
)
PAIR = 2 * OWN
ROWS = SLOTS * PAIR
HALF = SLOTS * OWN
MESH = pl.DeviceIdType.MESH
F32, BF16 = jnp.float32, jnp.bfloat16


def dot(a, b):
    return jnp.dot(a, b, preferred_element_type=F32)


def split(a):
    high = a.astype(BF16)
    return high, (a - high.astype(F32)).astype(BF16)


def far_first(k):
    return lax.rem(4 + (1 - 2 * lax.rem(k, 2)) * lax.div(k + 1, 2) + 8, 8)


def kernel(
    samples_h, opacity_h, counts_h, order_h, target_h, first_h, second_h,
    pixels_o, grad_in_o, grad_out_o,
    xs, op, cnt, order, tgt, w1, w2,
    passed, near, ct, vt, vc, spread_veil, w2t, hid, total, sums, wsend, wrecv, pgs, fst, gin, gout,
    grads, shares,
    load_sem, chunk_sem, n_send, n_recv, p_send, p_recv, w_send, w_recv, g_send, g_recv, f_send, f_recv,
    e_send, e_recv, met,
):
    tile = lax.axis_index("tile")
    own = lax.axis_index("depth")
    zi, core = lax.div(own, 2), lax.rem(own, 2)
    xi, yi = lax.div(tile, YS), lax.rem(tile, YS)
    partner = 2 * zi + 1 - core

    barrier = pltpu.get_barrier_semaphore()

    def greet(t, d):
        pl.semaphore_signal(
            barrier, inc=1, device_id={"tile": t, "depth": d}, device_id_type=MESH
        )

    for j in (8, 9, 7, 10, 6, 11, 5, 12, 4, 13, 3, 14, 2, 15, 1):
        greet(tile, lax.rem(own + j, BRICKS))
    for j in range(1, XS):
        greet(lax.rem(xi + j, XS) * YS + yi, own)
    for j in range(1, YS):
        greet(xi * YS + lax.rem(yi + j, YS), own)

    loads = [
        pltpu.make_async_copy(a, b, load_sem.at[i])
        for i, (a, b) in enumerate(
            [
                (opacity_h.at[0], op), (counts_h, cnt), (first_h.at[0], w1),
                (second_h.at[0], w2), (order_h, order), (target_h, tgt),
            ]
        )
    ]
    for load in loads[:3]:
        load.start()

    def rays_of(zt):
        return pl.ds(pl.multiple_of(zt * PAIR, PAIR), PAIR)

    def fetch(k):
        rays = rays_of(lax.rem(zi + FAR[k], ZS))
        return pltpu.make_async_copy(samples_h.at[0, :, rays, :], xs.at[:, rays, :], chunk_sem.at[k])

    for k in range(ZS):
        fetch(k).start()
    for load in loads[3:]:
        load.start()

    def remote(src, dst, send, recv, t, d):
        return pltpu.make_async_remote_copy(
            src_ref=src, dst_ref=dst, send_sem=send, recv_sem=recv,
            device_id={"tile": t, "depth": d}, device_id_type=MESH,
        )

    loads[0].wait()
    loads[1].wait()
    slot = lax.broadcasted_iota(jnp.int32, (SLOTS, RAYS), 0)
    living = jnp.where(slot < cnt[...], 1.0, 0.0).astype(F32)
    alpha = op[...] * living
    kept = 1.0 - alpha
    through = jnp.ones((1, RAYS), F32)
    rows = []
    for s in range(SLOTS):
        rows.append(alpha[s : s + 1] * through)
        through = through * kept[s : s + 1]
    contrib = jnp.concatenate(rows + [jnp.zeros((128 - SLOTS, RAYS), F32)], axis=0)
    for q in range(4):
        passed[own, q] = through[:, 128 * q : 128 * q + 128]
    ct[...] = contrib.T

    def all_of(ref, count, sem):
        part = ref.at[pl.ds(0, count)]
        pltpu.make_async_copy(part, part, sem).wait()

    def n_copy(d):
        return remote(
            passed.at[own, lax.div(d, 4)], near.at[own], n_send, n_recv, tile, d
        )

    def p_copy(d):
        return remote(passed.at[own], passed.at[own], p_send, p_recv, tile, d)

    loads[2].wait()
    loads[3].wait()

    def w_copy(d):
        return remote(wsend.at[d], wrecv.at[own], w_send, w_recv, tile, d)

    def forward(targets):
        acts = [
            jnp.maximum(dot(xs[:, rays_of(zt), :].reshape(ROWS, ENC), w1[...]), 0.0)
            for zt in targets
        ]
        accs = []
        for zt, act in zip(targets, acts):
            cols = ct[rays_of(zt), :]
            acc = jnp.zeros((PAIR, HID), F32)
            for s in range(SLOTS):
                acc = acc + act[s * PAIR : (s + 1) * PAIR] * cols[:, s : s + 1]
            accs.append(acc)
        terms = []
        for acc in accs:
            high, low = split(acc)
            terms.append(dot(high, w2[...]) + dot(low, w2[...]))
        for zt, act, acc, term in zip(targets, acts, accs, terms):
            wsend[pl.ds(2 * zt, 2)] = term.reshape(2, OWN, FEAT)
            total[rays_of(zt), :] = acc
            rounded = act.astype(BF16).reshape(SLOTS, 2, OWN, HID)
            for c in range(2):
                hid[c, zt] = rounded[:, c].reshape(HALF, HID)

    def send_pair(zt):
        w_copy(2 * zt).start()
        w_copy(2 * zt + 1).start()

    targets = [lax.rem(zi + off, ZS) for off in FAR]

    def compute(k):
        fetch(2 * k).wait()
        fetch(2 * k + 1).wait()
        forward(targets[2 * k : 2 * k + 2])

    for k in range(EARLY):
        compute(k)

    pl.semaphore_wait(barrier, BRICKS - 1 + XS - 1 + YS - 1)

    for j in (8, 9, 7, 10, 6, 11, 5, 12, 4, 13, 3, 14, 2, 15, 1):
        n_copy(lax.rem(own + j, BRICKS)).start()
    for zt in targets[: 2 * EARLY]:
        send_pair(zt)
    for k in range(EARLY, 4):
        compute(k)
        for zt in targets[2 * k : 2 * k + 2][: 2 if k < 3 else 1]:
            send_pair(zt)

    w_copy(partner).start()
    wrecv[own] = wsend[own]
    near[own] = passed[own, lax.div(own, 4)]

    for j in range(1, XS):
        pl.semaphore_signal(
            met, inc=1,
            device_id={"tile": lax.rem(xi + j, XS) * YS + yi, "depth": own},
            device_id_type=MESH,
        )

    @pl.loop(0, ZS - 1)
    def _(k):
        zt = lax.rem(zi + far_first(k), ZS)
        p_copy(2 * zt).start()
        p_copy(2 * zt + 1).start()

    p_copy(partner).start()

    @pl.loop(0, ZS)
    def _(zt):
        rays = rays_of(zt)
        cols = ct[rays, :]
        parts = []
        for s in range(SLOTS):
            parts.append((xs[s, rays, :].astype(F32) * cols[:, s : s + 1]).astype(BF16))
        for c in range(2):
            half = jnp.concatenate([part[c * OWN : c * OWN + OWN] for part in parts], axis=0)
            fst[c, zt] = half.T

    loads[4].wait()
    loads[5].wait()

    all_of(near, BRICKS - 1, n_recv)

    rank = order[...].astype(F32)
    grid = (BRICKS, BRICKS)
    ranks = jnp.broadcast_to(rank, grid)
    row, col = (lax.broadcasted_iota(jnp.int32, grid, i) for i in range(2))
    rank_col = jnp.sum(jnp.where(row == col, ranks, 0.0), axis=1, keepdims=True)
    own_rank = jnp.sum(jnp.where(col[:1] == own, rank, 0.0), axis=1, keepdims=True)

    def product(ahead, every):
        chosen = jnp.where(rank_col < ahead, every, 1.0)
        chosen = chosen[:8] * chosen[8:]
        chosen = chosen[:4] * chosen[4:]
        chosen = chosen[:2] * chosen[2:]
        return chosen[:1] * chosen[1:]

    every = jnp.concatenate([near[b] for b in range(BRICKS)], axis=0)
    veils = [product(rank[:, b : b + 1], every) for b in range(BRICKS)]
    vt[...] = jnp.concatenate(veils + [jnp.zeros((128 - BRICKS, 128), F32)], axis=0).T
    mine = vt[pl.ds(pl.multiple_of(lax.rem(own, 4) * OWN, OWN), OWN), :]
    for b in range(BRICKS):
        spread_veil[b] = jnp.broadcast_to(mine[:, b : b + 1], (OWN, FEAT))
    w2t[...] = w2[...].T

    all_of(wrecv, BRICKS - 1, w_recv)

    lanes = [jnp.zeros((OWN, FEAT), F32)] * 2
    for b in range(BRICKS):
        lanes[b % 2] = lanes[b % 2] + wrecv[b] * spread_veil[b]
    pixels = lanes[0] + lanes[1]
    pixels_o[...] = pixels
    pgs[own] = pixels - tgt[...]

    def g_copy(d):
        return remote(pgs.at[own], pgs.at[own], g_send, g_recv.at[zi], tile, d)

    def f_copy(b):
        return remote(pgs.at[b], pgs.at[b], f_send, f_recv, tile, partner)

    @pl.loop(0, ZS - 1)
    def _(k):
        g_copy(2 * lax.rem(zi + far_first(k), ZS) + core).start()

    g_copy(partner).start()

    all_of(passed, BRICKS - 1, p_recv)

    for q in range(4):
        every = jnp.concatenate([passed[b, q] for b in range(BRICKS)], axis=0)
        veil = product(own_rank, every)
        vc[128 * q : 128 * q + 128, :] = jnp.broadcast_to(veil, (128, 128)).T

    for c in range(2):
        half = jnp.concatenate(
            [total[PAIR * z + OWN * c : PAIR * z + OWN * c + OWN, :] for z in range(ZS)], axis=0
        )
        sums[c] = half.T.astype(BF16)

    all_of(near, BRICKS - 1, n_send)
    all_of(passed, BRICKS - 1, p_send)
    all_of(wsend, BRICKS - 1, w_send)

    def wait_g(b):
        pltpu.make_async_copy(pgs.at[b], pgs.at[b], g_recv.at[lax.div(b, 2)]).wait()

    def gradient(c):
        grads = jnp.concatenate([pgs[2 * z + c] for z in range(ZS)], axis=0)
        cols = [vc[pl.ds(pl.multiple_of(PAIR * z + OWN * c, OWN), OWN), :] for z in range(ZS)]
        high, low = split(grads * jnp.concatenate(cols, axis=0))
        return high, (dot(high, w2t[...]) + dot(low, w2t[...])).astype(BF16)

    def grad_in_of(c, spread):
        acc = jnp.zeros((ENC, HID), F32)
        for z in range(ZS):
            mine = spread[OWN * z : OWN * z + OWN]
            parts = []
            for s in range(SLOTS):
                live = hid[c, z, s * OWN : s * OWN + OWN, :] > 0
                parts.append(jnp.where(live, mine, jnp.zeros_like(mine)))
            acc = acc + dot(fst[c, z], jnp.concatenate(parts, axis=0))
        return acc

    for k in range(ZS - 1):
        b = 2 * lax.rem(zi + far_first(6 - k), ZS) + core
        wait_g(b)
        f_copy(b).start()

    high, spread = gradient(core)
    gout[...] = dot(sums[core], high)
    gin[...] = grad_in_of(core, spread)

    wait_g(partner)
    all_of(pgs, ZS - 1, f_recv)

    high, spread = gradient(1 - core)
    gout_total = gout[...] + dot(sums[1 - core], high)

    def tile_at(dx, dy):
        return lax.rem(xi + dx, XS) * YS + lax.rem(yi + dy, YS)

    def e_copy(i, t):
        return remote(grads.at[i, t], shares.at[i, tile], e_send.at[i], e_recv.at[i], t, own)

    def scatter(i):
        for dx, dy in FAR_TILES:
            e_copy(i, tile_at(dx, dy)).start()

    grads[0] = gout_total.reshape(TILES, 8, FEAT)
    pl.semaphore_wait(met, XS - 1)
    scatter(0)
    total_in = gin[...] + grad_in_of(1 - core, spread)
    for t in range(TILES):
        rows = total_in[4 * t : 4 * t + 4]
        grads[1, t] = jnp.concatenate([rows[:, :128], rows[:, 128:]], axis=0)
    scatter(1)
    for i in range(2):
        shares[i, tile] = grads[i, tile]
    all_of(pgs, ZS, g_send)
    all_of(pgs, ZS - 1, f_send)
    for i in range(2):
        all_of(shares.at[i], TILES - 1, e_recv.at[i])
    acc_out, acc_in = shares[0, 0], shares[1, 0]
    for t in range(1, TILES):
        acc_out = acc_out + shares[0, t]
        acc_in = acc_in + shares[1, t]
    grad_out_o[0] = acc_out
    grad_in_o[0] = jnp.concatenate([acc_in[:4], acc_in[4:]], axis=1)
    for i in range(2):
        all_of(grads.at[i], TILES - 1, e_send.at[i])


def write(pixels, grad_in, grad_out, pixels_o, grad_in_o, grad_out_o, sem):
    copies = [
        pltpu.make_async_copy(a, b, sem.at[i])
        for i, (a, b) in enumerate(
            [(pixels, pixels_o), (grad_in, grad_in_o), (grad_out, grad_out_o)]
        )
    ]
    for copy in copies:
        copy.start()
    for copy in copies:
        copy.wait()


def per_device(samples, opacity, counts, depth_order, target, weight_in, weight_out):
    in_hbm = pl.BlockSpec(memory_space=pltpu.HBM)
    vmem = pl.BlockSpec(memory_space=pltpu.VMEM)
    dma = pltpu.SemaphoreType.DMA
    shapes = (
        jax.ShapeDtypeStruct((OWN, FEAT), F32),
        jax.ShapeDtypeStruct((1, 4, HID), F32),
        jax.ShapeDtypeStruct((1, 8, FEAT), F32),
    )
    results = pl.pallas_call(
        kernel,
        out_shape=shapes,
        in_specs=[in_hbm] * 7,
        out_specs=(vmem, vmem, vmem),
        scratch_shapes=[
            pltpu.VMEM((SLOTS, RAYS, ENC), BF16),
            pltpu.VMEM((SLOTS, RAYS), F32),
            pltpu.VMEM((1, RAYS), jnp.int32),
            pltpu.VMEM((1, BRICKS), jnp.int32),
            pltpu.VMEM((OWN, FEAT), F32),
            pltpu.VMEM((ENC, HID), BF16),
            pltpu.VMEM((HID, FEAT), BF16),
            pltpu.VMEM((BRICKS, 4, 1, 128), F32),
            pltpu.VMEM((BRICKS, 1, 128), F32),
            pltpu.VMEM((RAYS, 128), F32),
            pltpu.VMEM((128, 128), F32),
            pltpu.VMEM((RAYS, 128), F32),
            pltpu.VMEM((BRICKS, OWN, FEAT), F32),
            pltpu.VMEM((FEAT, HID), BF16),
            pltpu.VMEM((2, ZS, HALF, HID), BF16),
            pltpu.VMEM((RAYS, HID), F32),
            pltpu.VMEM((2, HID, RAYS // 2), BF16),
            pltpu.VMEM((BRICKS, OWN, FEAT), F32),
            pltpu.VMEM((BRICKS, OWN, FEAT), F32),
            pltpu.VMEM((BRICKS, OWN, FEAT), F32),
            pltpu.VMEM((2, ZS, ENC, HALF), BF16),
            pltpu.VMEM((ENC, HID), F32),
            pltpu.VMEM((HID, FEAT), F32),
            pltpu.VMEM((2, TILES, 8, 128), F32),
            pltpu.VMEM((2, TILES, 8, 128), F32),
            dma((6,)), dma((ZS,)),
            dma(()), dma(()), dma(()), dma(()), dma(()), dma(()),
            dma(()), dma((ZS,)), dma(()), dma(()),
            dma((2,)), dma((2,)), pltpu.SemaphoreType.REGULAR,
        ],
        compiler_params=pltpu.CompilerParams(
            collective_id=0, has_side_effects=True, vmem_limit_bytes=32 * 2**20
        ),
        name="field_step",
    )(*(
        pltpu.with_memory_space_constraint(a, pltpu.HBM)
        for a in (samples, opacity, counts, depth_order, target, weight_in, weight_out)
    ))
    return pl.pallas_call(
        write,
        out_shape=shapes,
        in_specs=[vmem] * 3,
        out_specs=(in_hbm,) * 3,
        scratch_shapes=[dma((3,))],
        compiler_params=pltpu.CompilerParams(vmem_limit_bytes=2**20),
        name="write_results",
    )(*results)


def solution(mesh):
    placed = (
        P("depth", None, "tile", None),
        P("depth", None, "tile"),
        P("depth", "tile"),
        P("tile", None),
        P(("tile", "depth"), None),
        P("depth", None, None),
        P("depth", None, None),
    )
    return jax.shard_map(
        per_device,
        mesh=mesh,
        in_specs=placed,
        out_specs=(P(("tile", "depth"), None), P("depth", "tile", None), P("depth", "tile", None)),
        check_vma=False,
    )
```

```python
import jax
import jax.numpy as jnp
from jax import lax
from jax.experimental import pallas as pl
from jax.experimental.pallas import tpu as pltpu
from jax.sharding import PartitionSpec as P

ENC, HID, FEAT, SLOTS, RAYS = 128, 256, 128, 16, 512
BRICKS, OWN = 16, 32
EARLY = 2
FAR = (4, 3, 5, 2, 6, 1, 7, 0)
ZS, XS, YS = 8, 4, 8
TILES = XS * YS
FAR_TILES = sorted(
    [(x, y) for x in range(XS) for y in range(YS) if x + y],
    key=lambda d: -min(d[0], XS - d[0]) - min(d[1], YS - d[1]),
)
PAIR = 2 * OWN
ROWS = SLOTS * PAIR
HALF = SLOTS * OWN
MESH = pl.DeviceIdType.MESH
F32, BF16 = jnp.float32, jnp.bfloat16


def dot(a, b):
    return jnp.dot(a, b, preferred_element_type=F32)


def split(a):
    high = a.astype(BF16)
    return high, (a - high.astype(F32)).astype(BF16)


def far_first(k):
    return lax.rem(4 + (1 - 2 * lax.rem(k, 2)) * lax.div(k + 1, 2) + 8, 8)


def kernel(
    samples_h, opacity_h, counts_h, order_h, target_h, first_h, second_h,
    pixels_o, grad_in_o, grad_out_o,
    xs, op, cnt, order, tgt, w1, w2,
    passed, near, ct, vt, vc, spread_veil, w2t, hid, total, sums, wsend, wrecv, pgs, fst, gin, gout,
    grads, shares,
    load_sem, chunk_sem, n_send, n_recv, p_send, p_recv, w_send, w_recv, g_send, g_recv, f_send, f_recv,
    e_send, e_recv, met,
):
    tile = lax.axis_index("tile")
    own = lax.axis_index("depth")
    zi, core = lax.div(own, 2), lax.rem(own, 2)
    xi, yi = lax.div(tile, YS), lax.rem(tile, YS)
    partner = 2 * zi + 1 - core

    barrier = pltpu.get_barrier_semaphore()

    def greet(t, d):
        pl.semaphore_signal(
            barrier, inc=1, device_id={"tile": t, "depth": d}, device_id_type=MESH
        )

    for j in (8, 9, 7, 10, 6, 11, 5, 12, 4, 13, 3, 14, 2, 15, 1):
        greet(tile, lax.rem(own + j, BRICKS))
    for j in range(1, XS):
        greet(lax.rem(xi + j, XS) * YS + yi, own)
    for j in range(1, YS):
        greet(xi * YS + lax.rem(yi + j, YS), own)

    loads = [
        pltpu.make_async_copy(a, b, load_sem.at[i])
        for i, (a, b) in enumerate(
            [
                (opacity_h.at[0], op), (counts_h, cnt), (first_h.at[0], w1),
                (second_h.at[0], w2), (order_h, order), (target_h, tgt),
            ]
        )
    ]
    for load in loads[:3]:
        load.start()

    def rays_of(zt):
        return pl.ds(pl.multiple_of(zt * PAIR, PAIR), PAIR)

    def fetch(k):
        rays = rays_of(lax.rem(zi + FAR[k], ZS))
        return pltpu.make_async_copy(samples_h.at[0, :, rays, :], xs.at[:, rays, :], chunk_sem.at[k // 2])

    for k in range(ZS):
        fetch(k).start()
    for load in loads[3:]:
        load.start()

    def remote(src, dst, send, recv, t, d):
        return pltpu.make_async_remote_copy(
            src_ref=src, dst_ref=dst, send_sem=send, recv_sem=recv,
            device_id={"tile": t, "depth": d}, device_id_type=MESH,
        )

    loads[0].wait()
    loads[1].wait()
    slot = lax.broadcasted_iota(jnp.int32, (SLOTS, RAYS), 0)
    living = jnp.where(slot < cnt[...], 1.0, 0.0).astype(F32)
    alpha = op[...] * living
    kept = 1.0 - alpha
    through = jnp.ones((1, RAYS), F32)
    rows = []
    for s in range(SLOTS):
        rows.append(alpha[s : s + 1] * through)
        through = through * kept[s : s + 1]
    contrib = jnp.concatenate(rows + [jnp.zeros((128 - SLOTS, RAYS), F32)], axis=0)
    for q in range(4):
        passed[own, q] = through[:, 128 * q : 128 * q + 128]
    ct[...] = contrib.T

    def all_of(ref, count, sem):
        part = ref.at[pl.ds(0, count)]
        pltpu.make_async_copy(part, part, sem).wait()

    def n_copy(d):
        return remote(
            passed.at[own, lax.div(d, 4)], near.at[own], n_send, n_recv, tile, d
        )

    def p_copy(d):
        return remote(passed.at[own], passed.at[own], p_send, p_recv, tile, d)

    loads[2].wait()
    loads[3].wait()

    def w_copy(d):
        return remote(wsend.at[d], wrecv.at[own], w_send, w_recv, tile, d)

    def forward(targets):
        acts = [
            jnp.maximum(dot(xs[:, rays_of(zt), :].reshape(ROWS, ENC), w1[...]), 0.0)
            for zt in targets
        ]
        accs = []
        for zt, act in zip(targets, acts):
            cols = ct[rays_of(zt), :]
            acc = jnp.zeros((PAIR, HID), F32)
            for s in range(SLOTS):
                acc = acc + act[s * PAIR : (s + 1) * PAIR] * cols[:, s : s + 1]
            accs.append(acc)
        terms = []
        for acc in accs:
            high, low = split(acc)
            terms.append(dot(high, w2[...]) + dot(low, w2[...]))
        for zt, act, acc, term in zip(targets, acts, accs, terms):
            wsend[pl.ds(2 * zt, 2)] = term.reshape(2, OWN, FEAT)
            total[rays_of(zt), :] = acc
            rounded = act.astype(BF16).reshape(SLOTS, 2, OWN, HID)
            for c in range(2):
                hid[c, zt] = rounded[:, c].reshape(HALF, HID)

    def send_pair(zt):
        w_copy(2 * zt).start()
        w_copy(2 * zt + 1).start()

    targets = [lax.rem(zi + off, ZS) for off in FAR]

    def compute(k):
        both = xs.at[:, pl.ds(0, 2 * PAIR), :]
        pltpu.make_async_copy(both, both, chunk_sem.at[k]).wait()
        forward(targets[2 * k : 2 * k + 2])

    for k in range(EARLY):
        compute(k)

    pl.semaphore_wait(barrier, BRICKS - 1 + XS - 1 + YS - 1)

    for j in (8, 9, 7, 10, 6, 11, 5, 12, 4, 13, 3, 14, 2, 15, 1):
        n_copy(lax.rem(own + j, BRICKS)).start()
    for zt in targets[: 2 * EARLY]:
        send_pair(zt)
    for k in range(EARLY, 4):
        compute(k)
        for zt in targets[2 * k : 2 * k + 2][: 2 if k < 3 else 1]:
            send_pair(zt)

    w_copy(partner).start()
    wrecv[own] = wsend[own]
    near[own] = passed[own, lax.div(own, 4)]

    for j in range(1, XS):
        pl.semaphore_signal(
            met, inc=1,
            device_id={"tile": lax.rem(xi + j, XS) * YS + yi, "depth": own},
            device_id_type=MESH,
        )

    @pl.loop(0, ZS - 1)
    def _(k):
        zt = lax.rem(zi + far_first(k), ZS)
        p_copy(2 * zt).start()
        p_copy(2 * zt + 1).start()

    p_copy(partner).start()

    @pl.loop(0, ZS)
    def _(zt):
        rays = rays_of(zt)
        cols = ct[rays, :]
        parts = []
        for s in range(SLOTS):
            parts.append((xs[s, rays, :].astype(F32) * cols[:, s : s + 1]).astype(BF16))
        for c in range(2):
            half = jnp.concatenate([part[c * OWN : c * OWN + OWN] for part in parts], axis=0)
            fst[c, zt] = half.T

    loads[4].wait()
    loads[5].wait()

    all_of(near, BRICKS - 1, n_recv)

    rank = order[...].astype(F32)
    grid = (BRICKS, BRICKS)
    ranks = jnp.broadcast_to(rank, grid)
    row, col = (lax.broadcasted_iota(jnp.int32, grid, i) for i in range(2))
    rank_col = jnp.sum(jnp.where(row == col, ranks, 0.0), axis=1, keepdims=True)
    own_rank = jnp.sum(jnp.where(col[:1] == own, rank, 0.0), axis=1, keepdims=True)

    def product(ahead, every):
        chosen = jnp.where(rank_col < ahead, every, 1.0)
        chosen = chosen[:8] * chosen[8:]
        chosen = chosen[:4] * chosen[4:]
        chosen = chosen[:2] * chosen[2:]
        return chosen[:1] * chosen[1:]

    every = jnp.concatenate([near[b] for b in range(BRICKS)], axis=0)
    veils = [product(rank[:, b : b + 1], every) for b in range(BRICKS)]
    vt[...] = jnp.concatenate(veils + [jnp.zeros((128 - BRICKS, 128), F32)], axis=0).T
    mine = vt[pl.ds(pl.multiple_of(lax.rem(own, 4) * OWN, OWN), OWN), :]
    for b in range(BRICKS):
        spread_veil[b] = jnp.broadcast_to(mine[:, b : b + 1], (OWN, FEAT))
    w2t[...] = w2[...].T

    all_of(wrecv, BRICKS - 1, w_recv)

    lanes = [jnp.zeros((OWN, FEAT), F32)] * 2
    for b in range(BRICKS):
        lanes[b % 2] = lanes[b % 2] + wrecv[b] * spread_veil[b]
    pixels = lanes[0] + lanes[1]
    pixels_o[...] = pixels
    pgs[own] = pixels - tgt[...]

    def g_copy(d):
        return remote(pgs.at[own], pgs.at[own], g_send, g_recv.at[zi], tile, d)

    def f_copy(b):
        return remote(pgs.at[b], pgs.at[b], f_send, f_recv, tile, partner)

    @pl.loop(0, ZS - 1)
    def _(k):
        g_copy(2 * lax.rem(zi + far_first(k), ZS) + core).start()

    g_copy(partner).start()

    all_of(passed, BRICKS - 1, p_recv)

    for q in range(4):
        every = jnp.concatenate([passed[b, q] for b in range(BRICKS)], axis=0)
        veil = product(own_rank, every)
        vc[128 * q : 128 * q + 128, :] = jnp.broadcast_to(veil, (128, 128)).T

    for c in range(2):
        half = jnp.concatenate(
            [total[PAIR * z + OWN * c : PAIR * z + OWN * c + OWN, :] for z in range(ZS)], axis=0
        )
        sums[c] = half.T.astype(BF16)

    all_of(near, BRICKS - 1, n_send)
    all_of(passed, BRICKS - 1, p_send)
    all_of(wsend, BRICKS - 1, w_send)

    def wait_g(b):
        pltpu.make_async_copy(pgs.at[b], pgs.at[b], g_recv.at[lax.div(b, 2)]).wait()

    def gradient(c):
        grads = jnp.concatenate([pgs[2 * z + c] for z in range(ZS)], axis=0)
        cols = [vc[pl.ds(pl.multiple_of(PAIR * z + OWN * c, OWN), OWN), :] for z in range(ZS)]
        high, low = split(grads * jnp.concatenate(cols, axis=0))
        return high, (dot(high, w2t[...]) + dot(low, w2t[...])).astype(BF16)

    def grad_in_of(c, spread):
        accs = [jnp.zeros((ENC, HID), F32)] * 2
        for z in range(ZS):
            mine = spread[OWN * z : OWN * z + OWN]
            parts = []
            for s in range(SLOTS):
                live = hid[c, z, s * OWN : s * OWN + OWN, :] > 0
                parts.append(jnp.where(live, mine, jnp.zeros_like(mine)))
            accs[z % 2] = accs[z % 2] + dot(fst[c, z], jnp.concatenate(parts, axis=0))
        return accs[0] + accs[1]

    for k in range(ZS - 1):
        b = 2 * lax.rem(zi + far_first(6 - k), ZS) + core
        wait_g(b)
        f_copy(b).start()

    high, spread = gradient(core)
    gout[...] = dot(sums[core], high)
    gin[...] = grad_in_of(core, spread)

    wait_g(partner)
    all_of(pgs, ZS - 1, f_recv)

    high, spread = gradient(1 - core)
    gout_total = gout[...] + dot(sums[1 - core], high)

    def tile_at(dx, dy):
        return lax.rem(xi + dx, XS) * YS + lax.rem(yi + dy, YS)

    def e_copy(i, t):
        return remote(grads.at[i, t], shares.at[i, tile], e_send.at[i], e_recv.at[i], t, own)

    def scatter(i):
        for dx, dy in FAR_TILES:
            e_copy(i, tile_at(dx, dy)).start()

    grads[0] = gout_total.reshape(TILES, 8, FEAT)
    pl.semaphore_wait(met, XS - 1)
    scatter(0)
    total_in = gin[...] + grad_in_of(1 - core, spread)
    for t in range(TILES):
        rows = total_in[4 * t : 4 * t + 4]
        grads[1, t] = jnp.concatenate([rows[:, :128], rows[:, 128:]], axis=0)
    scatter(1)
    for i in range(2):
        shares[i, tile] = grads[i, tile]
    all_of(pgs, ZS, g_send)
    all_of(pgs, ZS - 1, f_send)
    for i in range(2):
        all_of(shares.at[i], TILES - 1, e_recv.at[i])
    acc_out, acc_in = shares[0, 0], shares[1, 0]
    for t in range(1, TILES):
        acc_out = acc_out + shares[0, t]
        acc_in = acc_in + shares[1, t]
    grad_out_o[0] = acc_out
    grad_in_o[0] = jnp.concatenate([acc_in[:4], acc_in[4:]], axis=1)
    for i in range(2):
        all_of(grads.at[i], TILES - 1, e_send.at[i])


def write(pixels, grad_in, grad_out, pixels_o, grad_in_o, grad_out_o, sem):
    copies = [
        pltpu.make_async_copy(a, b, sem.at[i])
        for i, (a, b) in enumerate(
            [(pixels, pixels_o), (grad_in, grad_in_o), (grad_out, grad_out_o)]
        )
    ]
    for copy in copies:
        copy.start()
    for copy in copies:
        copy.wait()


def per_device(samples, opacity, counts, depth_order, target, weight_in, weight_out):
    in_hbm = pl.BlockSpec(memory_space=pltpu.HBM)
    vmem = pl.BlockSpec(memory_space=pltpu.VMEM)
    dma = pltpu.SemaphoreType.DMA
    shapes = (
        jax.ShapeDtypeStruct((OWN, FEAT), F32),
        jax.ShapeDtypeStruct((1, 4, HID), F32),
        jax.ShapeDtypeStruct((1, 8, FEAT), F32),
    )
    results = pl.pallas_call(
        kernel,
        out_shape=shapes,
        in_specs=[in_hbm] * 7,
        out_specs=(vmem, vmem, vmem),
        scratch_shapes=[
            pltpu.VMEM((SLOTS, RAYS, ENC), BF16),
            pltpu.VMEM((SLOTS, RAYS), F32),
            pltpu.VMEM((1, RAYS), jnp.int32),
            pltpu.VMEM((1, BRICKS), jnp.int32),
            pltpu.VMEM((OWN, FEAT), F32),
            pltpu.VMEM((ENC, HID), BF16),
            pltpu.VMEM((HID, FEAT), BF16),
            pltpu.VMEM((BRICKS, 4, 1, 128), F32),
            pltpu.VMEM((BRICKS, 1, 128), F32),
            pltpu.VMEM((RAYS, 128), F32),
            pltpu.VMEM((128, 128), F32),
            pltpu.VMEM((RAYS, 128), F32),
            pltpu.VMEM((BRICKS, OWN, FEAT), F32),
            pltpu.VMEM((FEAT, HID), BF16),
            pltpu.VMEM((2, ZS, HALF, HID), BF16),
            pltpu.VMEM((RAYS, HID), F32),
            pltpu.VMEM((2, HID, RAYS // 2), BF16),
            pltpu.VMEM((BRICKS, OWN, FEAT), F32),
            pltpu.VMEM((BRICKS, OWN, FEAT), F32),
            pltpu.VMEM((BRICKS, OWN, FEAT), F32),
            pltpu.VMEM((2, ZS, ENC, HALF), BF16),
            pltpu.VMEM((ENC, HID), F32),
            pltpu.VMEM((HID, FEAT), F32),
            pltpu.VMEM((2, TILES, 8, 128), F32),
            pltpu.VMEM((2, TILES, 8, 128), F32),
            dma((6,)), dma((ZS // 2,)),
            dma(()), dma(()), dma(()), dma(()), dma(()), dma(()),
            dma(()), dma((ZS,)), dma(()), dma(()),
            dma((2,)), dma((2,)), pltpu.SemaphoreType.REGULAR,
        ],
        compiler_params=pltpu.CompilerParams(
            collective_id=0, has_side_effects=True, vmem_limit_bytes=32 * 2**20
        ),
        name="field_step",
    )(*(
        pltpu.with_memory_space_constraint(a, pltpu.HBM)
        for a in (samples, opacity, counts, depth_order, target, weight_in, weight_out)
    ))
    return pl.pallas_call(
        write,
        out_shape=shapes,
        in_specs=[vmem] * 3,
        out_specs=(in_hbm,) * 3,
        scratch_shapes=[dma((3,))],
        compiler_params=pltpu.CompilerParams(vmem_limit_bytes=2**20),
        name="write_results",
    )(*results)


def solution(mesh):
    placed = (
        P("depth", None, "tile", None),
        P("depth", None, "tile"),
        P("depth", "tile"),
        P("tile", None),
        P(("tile", "depth"), None),
        P("depth", None, None),
        P("depth", None, None),
    )
    return jax.shard_map(
        per_device,
        mesh=mesh,
        in_specs=placed,
        out_specs=(P(("tile", "depth"), None), P("depth", "tile", None), P("depth", "tile", None)),
        check_vma=False,
    )
```
